8 devices in a mesh: dp: 2 (over y, z), tp: 4 (over x, core).
Axes of the slice: x: 2, y: 2, z: 1, core: 2. Of those that a mesh axis runs over, the one named last changes fastest.
Arguments:
- x: bfloat16 [4096, 2048], P(('dp', 'tp')), parts along dimension 0
- gain_a: bfloat16 [2048], replicated
- wq: bfloat16 [2048, 2048], P(None, 'tp')
- wk: bfloat16 [2048, 2048], P(None, 'tp')
- wv: bfloat16 [2048, 2048], P(None, 'tp')
- wo: bfloat16 [2048, 2048], P('tp')
- gain_m: bfloat16 [2048], replicated
- w_gate: bfloat16 [2048, 8192], P(None, 'tp')
- w_up: bfloat16 [2048, 8192], P(None, 'tp')
- w_down: bfloat16 [8192, 2048], P('tp')
Outputs:
- output: bfloat16 [4096, 2048], P(('dp', 'tp')), parts along dimension 0
There are 2 independent parts. The reference program is written for one: setup_inputs(seed, part) draws one part's arguments, and reference() takes and returns one part's arrays. A program takes and returns all parts, laid end to end along the dimension named above; an argument that names none is the same for every part.
All inputs are finite; a program needn't handle non-finite values.
Results may differ from the reference program's by a relative error of at most 0.017.
Values are sent between devices in bfloat16 or wider.
A program may use at most 2 GiB of HBM per device.

```python
import jax
import jax.numpy as jnp
from jax import lax

ROWS = 2048
D = 2048
HEADS = 16
KV_HEADS = 16
HEAD = 128
FF = 8192
THETA = 10000


def setup_inputs(seed: int = 0, part: int = 0) -> dict:
    kx, kn, kq, kk, kv, ko, km, kg, ku, kd = jax.random.split(jax.random.key(seed), 10)

    def weights(key, rows, columns):
        return jax.random.normal(key, (rows, columns), jnp.float32) * rows**-0.5

    drawn = {
        "x": jax.random.normal(jax.random.fold_in(kx, part), (ROWS, D), jnp.float32),
        "gain_a": 1 + 0.1 * jax.random.normal(kn, (D,), jnp.float32),
        "wq": 2 * weights(kq, D, HEADS * HEAD),
        "wk": 2 * weights(kk, D, KV_HEADS * HEAD),
        "wv": 4 * weights(kv, D, KV_HEADS * HEAD),
        "wo": weights(ko, HEADS * HEAD, D),
        "gain_m": 1 + 0.1 * jax.random.normal(km, (D,), jnp.float32),
        "w_gate": weights(kg, D, FF),
        "w_up": weights(ku, D, FF),
        "w_down": 2 * weights(kd, FF, D),
    }
    return {k: v.astype(jnp.bfloat16) for k, v in drawn.items()}


def normed(x, gain):
    wide = x.astype(jnp.float32)
    scale = lax.rsqrt(jnp.mean(wide * wide, -1, keepdims=True) + 1e-6)
    return (wide * scale * gain.astype(jnp.float32)).astype(jnp.bfloat16)


def turned(t, place, theta):
    half = t.shape[-1] // 2
    angle = place.astype(jnp.float32)[:, None] * theta ** (-jnp.arange(half, dtype=jnp.float32) / half)
    cos, sin = jnp.cos(angle)[:, None], jnp.sin(angle)[:, None]
    a, b = t[..., :half].astype(jnp.float32), t[..., half:].astype(jnp.float32)
    return jnp.concatenate([a * cos - b * sin, b * cos + a * sin], -1).astype(jnp.bfloat16)


def matmul(a, w):
    return jnp.dot(a, w, preferred_element_type=jnp.float32).astype(jnp.bfloat16)


def einsum(form, a, b):
    return jnp.einsum(form, a.astype(jnp.float32), b.astype(jnp.float32))


def attention(q, k, v):
    scores = einsum("tgsd,ugd->gstu", q, k) * q.shape[-1] ** -0.5
    token = jnp.arange(q.shape[0])
    scores = jnp.where(token[:, None] >= token, scores, -jnp.inf)
    weights = jax.nn.softmax(scores, -1).astype(jnp.bfloat16)
    return einsum("gstu,ugd->tgsd", weights, v).astype(jnp.bfloat16)


def reference(x, gain_a, wq, wk, wv, wo, gain_m, w_gate, w_up, w_down):
    a, place = normed(x, gain_a), jnp.arange(ROWS)
    q = turned(matmul(a, wq).reshape(ROWS, HEADS, HEAD), place, THETA).reshape(ROWS, KV_HEADS, -1, HEAD)
    k = turned(matmul(a, wk).reshape(ROWS, KV_HEADS, HEAD), place, THETA)
    v = matmul(a, wv).reshape(ROWS, KV_HEADS, HEAD)
    seen = attention(q, k, v).reshape(ROWS, HEADS * HEAD)
    h = (x.astype(jnp.float32) + jnp.dot(seen, wo, preferred_element_type=jnp.float32)).astype(jnp.bfloat16)
    b = normed(h, gain_m)
    gate = jnp.dot(b, w_gate, preferred_element_type=jnp.float32)
    up = jnp.dot(b, w_up, preferred_element_type=jnp.float32)
    hidden = (jax.nn.silu(gate) * up).astype(jnp.bfloat16)
    return (h.astype(jnp.float32) + jnp.dot(hidden, w_down, preferred_element_type=jnp.float32)).astype(jnp.bfloat16)
```

```python
import functools

import jax
import jax.numpy as jnp
import numpy as np
from jax import lax
from jax.experimental import pallas as pl
from jax.experimental.pallas import tpu as pltpu
from jax.sharding import PartitionSpec as P

HEAD = 128
HEADS = 4
BLOCK = 512
THETA = 10000
NEG = -1e30
HIDDEN = 2 * NEG
LOG2E = 1.4426950408889634
VMEM = 56 * 2**20
F32, BF16 = jnp.float32, jnp.bfloat16

SIB = [(0, 1), (1, 0), (2, 3), (3, 2)]
CROSS = [(0, 2), (2, 0), (1, 3), (3, 1)]
DIAG = [(0, 3), (3, 0), (1, 2), (2, 1)]


def _dot(a, b, ca=1, cb=0):
    return lax.dot_general(a, b, (((ca,), (cb,)), ((), ())), preferred_element_type=F32)


def _normed(x, gain):
    wide = x.astype(F32)
    scale = lax.rsqrt(jnp.mean(wide * wide, -1, keepdims=True) + 1e-6)
    return (wide * scale * gain.astype(F32)).astype(BF16)


def _call(body, ids, grid, ins, outs, scratch=(), flops=0, name=None, semantics=None, exps=0):
    specs = [pl.BlockSpec(i[1], i[2]) if isinstance(i, tuple) else pl.BlockSpec(memory_space=pl.ANY) for i in ins]
    arrays = [i[0] if isinstance(i, tuple) else i for i in ins]
    shapes = [jax.ShapeDtypeStruct(o[0], o[1]) for o in outs]
    moved = sum(a.size * a.dtype.itemsize for a in [*arrays, *shapes])
    return pl.pallas_call(
        body,
        grid_spec=pltpu.PrefetchScalarGridSpec(
            num_scalar_prefetch=1, grid=grid, in_specs=specs, out_specs=[pl.BlockSpec(o[2], o[3]) for o in outs], scratch_shapes=list(scratch)
        ),
        out_shape=shapes,
        compiler_params=pltpu.CompilerParams(dimension_semantics=("arbitrary",) * len(grid), vmem_limit_bytes=VMEM),
        cost_estimate=pl.CostEstimate(flops=flops, transcendentals=exps, bytes_accessed=moved),
        name=name,
    )(ids, *arrays)


def _table():
    half = HEAD // 2
    rate = np.float32(THETA) ** (-np.arange(half, dtype=np.float32) / np.float32(half))
    angle = np.arange(2048, dtype=np.float32)[:, None] * rate.astype(np.float32)
    return np.concatenate([np.cos(angle), np.sin(angle)], 1).astype(np.float32)


def _qkv_body(pieces, ids, *refs):
    xs, (gain, wq, wk, wv, tab, q_ref, k_ref, v_ref, a_s) = refs[:pieces], refs[pieces:]
    k = ids[1]

    @pl.when(pl.program_id(0) == 0)
    def _():
        for i, x in enumerate(xs):
            rows = BLOCK // pieces
            at = 0 if pieces == 1 else pl.multiple_of((k if i == 0 else 1 - k) * rows, rows)
            a_s[pl.ds(at, rows), :] = _normed(x[...], gain[...])

    t = tab[...]
    flip = pltpu.roll(t, HEAD // 2, 1)
    first = lax.broadcasted_iota(jnp.int32, t.shape, 1) < HEAD // 2
    cos, sin = jnp.where(first, t, flip), jnp.where(first, -flip, t)
    a = a_s[...]
    for w, out in ((wq, q_ref), (wk, k_ref)):
        y = _dot(a, w[...]).astype(BF16).astype(F32)
        for n in range(2):
            z = y[:, n * HEAD : (n + 1) * HEAD]
            out[n] = (z * cos + pltpu.roll(z, HEAD // 2, 1) * sin).astype(BF16)
    v = _dot(a, wv[...]).astype(BF16)
    for n in range(2):
        v_ref[n] = v[:, n * HEAD : (n + 1) * HEAD].T


def _qkv(ids, pieces, at, gain, wq, wk, wv, tab):
    n = len(pieces)
    whole = lambda i, ids: (0, 0)
    cols = lambda i, ids: (0, i)
    w = (2048, 2 * HEAD)
    q = ((HEADS, BLOCK, HEAD), BF16, (2, BLOCK, HEAD), lambda i, ids: (i, 0, 0))
    v = ((HEADS, HEAD, BLOCK), BF16, (2, HEAD, BLOCK), lambda i, ids: (i, 0, 0))
    return _call(
        functools.partial(_qkv_body, n), ids, (2,),
        [*[(x, (BLOCK // n, 2048), whole) for x in pieces], (gain, (1, 2048), whole), (wq, w, cols), (wk, w, cols), (wv, w, cols),
         (tab, (BLOCK, HEAD), lambda i, ids: (at(ids), 0))],
        [q, q, v], [pltpu.VMEM((BLOCK, 2048), BF16)], flops=2 * BLOCK * 2048 * 1536, name="qkv")


E = HEAD**-0.5 * LOG2E


def _scores(q, k, diagonal):
    s = _dot(k, q, 1, 1)
    if diagonal:
        s = jnp.where(lax.broadcasted_iota(jnp.int32, s.shape, 1) >= lax.broadcasted_iota(jnp.int32, s.shape, 0), s, HIDDEN)
    return s


def _tasks(tasks):
    scores = [_scores(q, k, d) for q, k, _, d in tasks]
    out = []
    for (_, _, v, _), s in zip(tasks, scores):
        top = s.max(axis=0, keepdims=True)
        p = jnp.exp2((s - top) * E).astype(BF16)
        out.append((p, top))
    ones = jnp.ones((8, BLOCK), BF16)
    return [(_dot(jnp.concatenate([v, ones], 0), p), top) for (_, _, v, _), (p, top) in zip(tasks, out)]


def _merge(parts):
    top = functools.reduce(jnp.maximum, [t for _, t in parts])
    return sum(a * jnp.exp2((t - top) * E) for a, t in parts), top


def _if(ok, part):
    return part[0], jnp.where(ok, part[1], NEG)


def _ended(part):
    acc = part[0]
    return (acc[:HEAD] * (1 / acc[HEAD : HEAD + 1])).T.astype(BF16)


def _pair(k, me, sib, n):
    a, b = me[n], sib[n]
    return jnp.where(k == 0, a, b), jnp.where(k == 0, b, a)


HB = 2


def _own_body(ids, qm, qs, km, ks, vm, vs, acc_ref, top_ref):
    k = ids[1]
    tasks = []
    for n in range(HB):
        q, kk, v = _pair(k, qm, qs, n), _pair(k, km, ks, n), _pair(k, vm, vs, n)
        tasks += [(q[0], kk[0], v[0], True), (q[1], kk[0], v[0], False), (q[1], kk[1], v[1], True)]
    done = _tasks(tasks)
    for n in range(HB):
        a, b, c = done[3 * n : 3 * n + 3]
        for j, (acc, top) in enumerate((a, _merge([b, c]))):
            acc_ref[n, j], top_ref[n, j] = acc, top


def _o0_body(ids, qm, qs, km, ks, vm, vs, q0, k0, v0, acc_in, top_in, acc_ref, top_ref, seen_ref):
    c, k = ids[0], ids[1]
    late = c == 0
    tasks = []
    for n in range(HB):
        q, kk, v = _pair(k, qm, qs, n), _pair(k, km, ks, n), _pair(k, vm, vs, n)
        tasks += [(q0[n], k0[n], v0[n], True)]
        for j in range(2):
            tasks += [(jnp.where(late, q0[n], q[j]), jnp.where(late, kk[j], k0[n]), jnp.where(late, v[j], v0[n]), False)]
    done = _tasks(tasks)
    for n in range(HB):
        d, *f = done[3 * n : 3 * n + 3]
        seen_ref[:, n * HEAD : (n + 1) * HEAD] = _ended(_merge([d, _if(late, f[0]), _if(late, f[1])]))
        for j in range(2):
            acc_ref[n, j], top_ref[n, j] = _merge([(acc_in[n, j], top_in[n, j]), _if(c == 1, f[j])])


def _o1_body(ids, qm, qs, km, ks, vm, vs, q0, k0, v0, q1, k1, v1, acc_in, top_in, seen_in, *outs):
    own_m, own_s, oth_m, oth_s = outs[:2], outs[2:4], outs[4:6], outs[6:8]
    c, k = ids[0], ids[1]
    late = c == 0
    tasks = []
    for n in range(HB):
        q, kk, v = _pair(k, qm, qs, n), _pair(k, km, ks, n), _pair(k, vm, vs, n)
        tasks += [(q1[n], k1[n], v1[n], True), (q1[n], k0[n], v0[n], False)]
        for j in range(2):
            tasks += [(jnp.where(late, q1[n], q[j]), jnp.where(late, kk[j], k1[n]), jnp.where(late, v[j], v1[n]), False)]
    done = _tasks(tasks)

    def put(m, s, j, n, o):
        cols = slice(n * HEAD, (n + 1) * HEAD)
        half = BLOCK // 2
        lo, hi = o[:half], o[half:]
        for refs, rows, e in ((m, jnp.where(k == 0, lo, hi), k if j == 0 else 1 - k), (s, jnp.where(k == 0, hi, lo), 1 - k if j == 0 else k)):
            for p in range(2):
                refs[p][e, :, cols] = rows[p * 128 : (p + 1) * 128]

    for n in range(HB):
        d, z, *f = done[4 * n : 4 * n + 4]
        put(oth_m, oth_s, 0, n, seen_in[:, n * HEAD : (n + 1) * HEAD])
        put(oth_m, oth_s, 1, n, _ended(_merge([d, z, _if(late, f[0]), _if(late, f[1])])))
        for j in range(2):
            put(own_m, own_s, j, n, _ended(_merge([(acc_in[n, j], top_in[n, j]), _if(c == 1, f[j])])))


def _attend(body, ids, qkvs, state, seen, outs, tasks, name):
    one = lambda i, ids: (i, 0, 0)
    qk, v = (HB, BLOCK, HEAD), (HB, HEAD, BLOCK)
    ins = []
    if len(qkvs) >= 2:
        for i in range(3):
            ins += [(t[i], v if i == 2 else qk, one) for t in qkvs[:2]]
    for t in qkvs[2:]:
        ins += [(t[0], qk, one), (t[1], qk, one), (t[2], v, one)]
    if state is not None:
        ins += [(state[0], (HB, 2, HEAD + 8, BLOCK), lambda i, ids: (i, 0, 0, 0)), (state[1], (HB, 2, 1, BLOCK), lambda i, ids: (i, 0, 0, 0))]
    if seen is not None:
        ins += [(seen, (BLOCK, HB * HEAD), lambda i, ids: (0, i))]
    n = HEADS * tasks * BLOCK * BLOCK
    return _call(body, ids, (HEADS // HB,), ins, outs, flops=4 * n * HEAD * 2, exps=n, name=name)


STATE = [((HEADS, 2, HEAD + 8, BLOCK), F32, (HB, 2, HEAD + 8, BLOCK), lambda i, ids: (i, 0, 0, 0)),
         ((HEADS, 2, 1, BLOCK), F32, (HB, 2, 1, BLOCK), lambda i, ids: (i, 0, 0, 0))]
SEEN = ((BLOCK, HEADS * HEAD), BF16, (BLOCK, HB * HEAD), lambda i, ids: (0, i))
PIECE = ((2, 128, HEADS * HEAD), BF16, (2, 128, HB * HEAD), lambda i, ids: (0, 0, i))


def _wo_body(parts, ids, *refs):
    n = 4 * parts
    seen, (a0, a1, b0, b1), wo, (h_ref, w_s, sem) = refs[:n], refs[n : n + 4], refs[n + 4 : -3], refs[-3:]
    k, g = ids[1], ids[2]
    copies = []
    for i, w in enumerate(wo):
        if i < 2:
            at, rows = i * 512, 512
        else:
            who, what = divmod(i - 2, 4)
            half = g if what < 2 else 1 - g
            at, rows = pl.multiple_of((2 + who) * 512 + half * 256 + (what % 2) * 128, 128), 128
        copies.append(pltpu.make_async_copy(w, w_s.at[pl.ds(at, rows)], sem.at[i]))
    for c in copies:
        c.start()
    rows = parts * 128
    s = [jnp.concatenate([seen[4 * p + i][e] for e in range(2) for p in range(parts)], 0) for i in range(4)]
    for c in copies:
        c.wait()
    step = 512
    for at in range(0, 2048, step):
        cols = slice(at, at + step)
        total = sum(_dot(s[i], w_s[i * 512 : (i + 1) * 512, cols]) for i in range(4))
        x = [jnp.where(k == 0, u[:, cols], v[:, cols]).astype(F32) for u, v in ((a0, a1), (b0, b1))]
        for e in range(2):
            h_ref[e, :, cols] = (x[e] + total[e * rows : (e + 1) * rows]).astype(BF16)


def _wo(ids, seen, residual, wo):
    parts = len(seen)
    rows = parts * 128
    ins = [(t, (2, 128, 512), lambda i, ids: (0, 0, 0)) for part in seen for t in part]
    for x, at in residual:
        ins.append((x, (rows, 2048), functools.partial(lambda at, i, ids: (at, 0), at)))
    return _call(functools.partial(_wo_body, parts), ids, (1,), [*ins, *wo],
                 [((2, rows, 2048), BF16, (2, rows, 2048), lambda i, ids: (0, 0, 0))],
                 [pltpu.VMEM((2048, 2048), BF16), pltpu.SemaphoreType.DMA((len(wo),))], flops=2 * 2 * rows * 2048 * 2048, name="wo")[0]


TILE = 256


def _mlp_body(adds, last, ids, m, s, gain, wg, wu, wd, *rest):
    more, (out, b_s, total) = rest[: 1 if adds else 0], rest[-3:]
    rows = m.shape[1]
    f = pl.program_id(0)

    @pl.when(f == 0)
    def _():
        b_s[:rows, :] = _normed(m[0], gain[...])
        b_s[rows:, :] = _normed(s[0], gain[...])

    b = b_s[...]
    gate, up = _dot(b, wg[...]), _dot(b, wu[...])
    hidden = (gate * jax.nn.sigmoid(gate) * up).astype(BF16)
    term = _dot(hidden, wd[...])

    @pl.when(f == 0)
    def _():
        total[...] = term

    @pl.when(f > 0)
    def _():
        total[...] += term

    @pl.when(f == pl.num_programs(0) - 1)
    def _():
        for e, h in ((0, m), (1, s)):
            y = total[e * rows : (e + 1) * rows, :]
            if adds:
                y = y + more[0][1 - e].astype(F32)
            if last:
                y = y + h[0].astype(F32)
            out[e] = y.astype(out.dtype)


def _mlp(ids, m, s, gain, wg, wu, wd, add=None, last=False):
    rows = m[0].shape[1]
    pick = lambda t: (t[0], (1, rows, 2048), functools.partial(lambda at, f, ids: (at, 0, 0), t[1]))
    ins = [pick(m), pick(s), (gain, (1, 2048), lambda f, ids: (0, 0)), (wg, (2048, TILE), lambda f, ids: (0, f)),
           (wu, (2048, TILE), lambda f, ids: (0, f)), (wd, (TILE, 2048), lambda f, ids: (f, 0))]
    if add is not None:
        ins.append((add, (2, rows, 2048), lambda f, ids: (0, 0, 0)))
    return _call(functools.partial(_mlp_body, add is not None, last), ids, (2048 // TILE,), ins,
                 [((2, rows, 2048), F32 if last else BF16, (2, rows, 2048), lambda f, ids: (0, 0, 0))],
                 [pltpu.VMEM((2 * rows, 2048), BF16), pltpu.VMEM((2 * rows, 2048), F32)],
                 flops=2 * 2 * rows * 2048 * 2048 * 3, exps=2 * rows * 2048, name="mlp")[0]


def _end_body(ids, z, xa, xb, y):
    for p, x in enumerate((xa, xb)):
        rows = slice(p * 128, (p + 1) * 128)
        y[rows, :] = (z[0, rows, :] + x[0].astype(F32)).astype(BF16)


def _end(ids, z, xa, xb):
    half = lambda e, ids: (e, 0, 0)
    return _call(_end_body, ids, (2,), [(z, (1, 256, 2048), half), (xa, (1, 128, 2048), half), (xb, (1, 128, 2048), half)],
                 [((512, 2048), BF16, (256, 2048), lambda e, ids: (e + ids[1] - 2 * e * ids[1], 0))], flops=2 * 512 * 2048, name="end")[0]


def solution(mesh):
    def pp(t, perm):
        return lax.ppermute(t, "tp", perm)

    def over(t):
        return lax.ppermute(t, "dp", [(0, 1), (1, 0)])

    def step(x, gain_a, wq, wk, wv, wo, gain_m, w_gate, w_up, w_down):
        t, g = lax.axis_index("tp"), lax.axis_index("dp")
        c, k = t // 2, t % 2
        ids = jnp.stack([c, k, g]).astype(jnp.int32)
        gain_a, gain_m = gain_a[None], gain_m[None]
        tab = jnp.asarray(_table())
        even = k == 0

        lo, hi = x[:256], x[256:]
        xs_hi = pp(hi, SIB)
        xs = pp(x, SIB)
        r0 = pp(jnp.where(even, lo, xs_hi), CROSS)
        r1 = pp(jnp.where(even, xs[:256], hi), CROSS)

        wa = lax.dynamic_slice_in_dim(wo, 256 * g, 128, 0)
        wb = lax.dynamic_slice_in_dim(wo, 256 * g + 128, 128, 0)
        (wa, wb), _ = lax.optimization_barrier(((wa, wb), r1))
        wa, wb = pp(wa, CROSS), pp(wb, CROSS)
        ya, yb = over(wa), over(wb)
        cross_wo = [wa, wb, ya, yb]
        wos = [wo, pp(wo, SIB), *cross_wo, *[pp(w, SIB) for w in cross_wo]]

        weights = (gain_a, wq, wk, wv, tab)
        me = _qkv(ids, [x], lambda i: 2 * i[0] + i[1], *weights)
        sib = _qkv(ids, [xs], lambda i: 2 * i[0] + 1 - i[1], *weights)
        state = _attend(_own_body, ids, [me, sib], None, None, STATE, 3, "attn_own")
        o0 = _qkv(ids, [r0, pp(r0, SIB)], lambda i: 2 - 2 * i[0], *weights)
        *state, seen0 = _attend(_o0_body, ids, [me, sib, o0], state, None, [*STATE, SEEN], 3, "attn_o0")
        o1 = _qkv(ids, [r1, pp(r1, SIB)], lambda i: 3 - 2 * i[0], *weights)
        pieces = _attend(_o1_body, ids, [me, sib, o0, o1], state, seen0, [PIECE] * 8, 4, "attn_o1")
        own_m, own_s, oth_m, oth_s = (pieces[i : i + 2] for i in range(0, 8, 2))

        oth_seen = [(oth_m[p], pp(oth_s[p], SIB), pp(own_m[p], CROSS), pp(own_s[p], DIAG)) for p in range(2)]
        own_seen = [(own_m[p], pp(own_s[p], SIB), pp(oth_m[p], CROSS), pp(oth_s[p], DIAG)) for p in range(2)]
        h = [_wo(ids, [oth_seen[p]], [(r0, p), (r1, p), (r1, p), (r0, p)], wos) for p in range(2)]
        hs = [pp(t, SIB) for t in h]
        h_own = _wo(ids, own_seen, [(x, 0), (x, 1), (xs, 0), (xs, 1)], wos)
        hs_own = pp(h_own, SIB)

        mlp = functools.partial(_mlp, ids, gain=gain_m, wg=w_gate, wu=w_up, wd=w_down)
        away = [mlp((h[p], 1), (hs[p], 0)) for p in range(2)]
        away = [pp(t, SIB) for t in away]
        far = [pp(mlp((h[p], 0), (hs[p], 1), add=away[p]), CROSS) for p in range(2)]
        near = pp(mlp((h_own, 1), (hs_own, 0)), SIB)
        z = mlp((h_own, 0), (hs_own, 1), add=near, last=True)
        return _end(ids, z, *far)

    tokens, columns, rows_of = P(("dp", "tp"), None), P(None, "tp"), P("tp", None)
    return jax.shard_map(
        step,
        mesh=mesh,
        in_specs=(tokens, P(None), columns, columns, columns, rows_of, P(None), columns, columns, rows_of),
        out_specs=tokens,
        check_vma=False,
    )
```

```python
import functools

import jax
import jax.numpy as jnp
import numpy as np
from jax import lax
from jax.experimental import pallas as pl
from jax.experimental.pallas import tpu as pltpu
from jax.sharding import PartitionSpec as P

HEAD = 128
HEADS = 4
BLOCK = 512
THETA = 10000
NEG = -1e30
HIDDEN = 2 * NEG
LOG2E = 1.4426950408889634
VMEM = 56 * 2**20
F32, BF16 = jnp.float32, jnp.bfloat16

SIB = [(0, 1), (1, 0), (2, 3), (3, 2)]
CROSS = [(0, 2), (2, 0), (1, 3), (3, 1)]
DIAG = [(0, 3), (3, 0), (1, 2), (2, 1)]


def _dot(a, b, ca=1, cb=0):
    return lax.dot_general(a, b, (((ca,), (cb,)), ((), ())), preferred_element_type=F32)


def _normed(x, gain):
    wide = x.astype(F32)
    scale = lax.rsqrt(jnp.mean(wide * wide, -1, keepdims=True) + 1e-6)
    return (wide * scale * gain.astype(F32)).astype(BF16)


def _call(body, ids, grid, ins, outs, scratch=(), flops=0, name=None, semantics=None, exps=0):
    specs = [pl.BlockSpec(i[1], i[2]) if isinstance(i, tuple) else pl.BlockSpec(memory_space=pl.ANY) for i in ins]
    arrays = [i[0] if isinstance(i, tuple) else i for i in ins]
    shapes = [jax.ShapeDtypeStruct(o[0], o[1]) for o in outs]
    moved = sum(a.size * a.dtype.itemsize for a in [*arrays, *shapes])
    return pl.pallas_call(
        body,
        grid_spec=pltpu.PrefetchScalarGridSpec(
            num_scalar_prefetch=1, grid=grid, in_specs=specs, out_specs=[pl.BlockSpec(o[2], o[3]) for o in outs], scratch_shapes=list(scratch)
        ),
        out_shape=shapes,
        compiler_params=pltpu.CompilerParams(dimension_semantics=("arbitrary",) * len(grid), vmem_limit_bytes=VMEM),
        cost_estimate=pl.CostEstimate(flops=flops, transcendentals=exps, bytes_accessed=moved),
        name=name,
    )(ids, *arrays)


def _table():
    half = HEAD // 2
    rate = np.float32(THETA) ** (-np.arange(half, dtype=np.float32) / np.float32(half))
    angle = np.arange(2048, dtype=np.float32)[:, None] * rate.astype(np.float32)
    return np.concatenate([np.cos(angle), np.sin(angle)], 1).astype(np.float32)


def _qkv_body(pieces, ids, *refs):
    xs, (gain, wq, wk, wv, tab, q_ref, k_ref, v_ref, a_s) = refs[:pieces], refs[pieces:]
    k = ids[1]

    @pl.when(pl.program_id(0) == 0)
    def _():
        for i, x in enumerate(xs):
            rows = BLOCK // pieces
            at = 0 if pieces == 1 else pl.multiple_of((k if i == 0 else 1 - k) * rows, rows)
            a_s[pl.ds(at, rows), :] = _normed(x[...], gain[...])

    t = tab[...]
    flip = pltpu.roll(t, HEAD // 2, 1)
    first = lax.broadcasted_iota(jnp.int32, t.shape, 1) < HEAD // 2
    cos, sin = jnp.where(first, t, flip), jnp.where(first, -flip, t)
    a = a_s[...]
    for w, out in ((wq, q_ref), (wk, k_ref)):
        y = _dot(a, w[...]).astype(BF16).astype(F32)
        for n in range(2):
            z = y[:, n * HEAD : (n + 1) * HEAD]
            out[n] = (z * cos + pltpu.roll(z, HEAD // 2, 1) * sin).astype(BF16)
    v = _dot(a, wv[...]).astype(BF16)
    for n in range(2):
        v_ref[n] = v[:, n * HEAD : (n + 1) * HEAD].T


def _qkv(ids, pieces, at, gain, wq, wk, wv, tab):
    n = len(pieces)
    whole = lambda i, ids: (0, 0)
    cols = lambda i, ids: (0, i)
    w = (2048, 2 * HEAD)
    q = ((HEADS, BLOCK, HEAD), BF16, (2, BLOCK, HEAD), lambda i, ids: (i, 0, 0))
    v = ((HEADS, HEAD, BLOCK), BF16, (2, HEAD, BLOCK), lambda i, ids: (i, 0, 0))
    return _call(
        functools.partial(_qkv_body, n), ids, (2,),
        [*[(x, (BLOCK // n, 2048), whole) for x in pieces], (gain, (1, 2048), whole), (wq, w, cols), (wk, w, cols), (wv, w, cols),
         (tab, (BLOCK, HEAD), lambda i, ids: (at(ids), 0))],
        [q, q, v], [pltpu.VMEM((BLOCK, 2048), BF16)], flops=2 * BLOCK * 2048 * 1536, name="qkv")


E = HEAD**-0.5 * LOG2E


def _scores(q, k, diagonal):
    s = _dot(k, q, 1, 1)
    if diagonal:
        s = jnp.where(lax.broadcasted_iota(jnp.int32, s.shape, 1) >= lax.broadcasted_iota(jnp.int32, s.shape, 0), s, HIDDEN)
    return s


def _tasks(tasks):
    scores = [_scores(q, k, d) for q, k, _, d in tasks]
    out = []
    for (_, _, v, _), s in zip(tasks, scores):
        top = s.max(axis=0, keepdims=True)
        p = jnp.exp2((s - top) * E).astype(BF16)
        out.append((p, top))
    ones = jnp.ones((8, BLOCK), BF16)
    return [(_dot(jnp.concatenate([v, ones], 0), p), top) for (_, _, v, _), (p, top) in zip(tasks, out)]


def _merge(parts):
    top = functools.reduce(jnp.maximum, [t for _, t in parts])
    return sum(a * jnp.exp2((t - top) * E) for a, t in parts), top


def _if(ok, part):
    return part[0], jnp.where(ok, part[1], NEG)


def _ended(part):
    acc = part[0]
    return (acc[:HEAD] * (1 / acc[HEAD : HEAD + 1])).T.astype(BF16)


def _pair(k, me, sib, n):
    a, b = me[n], sib[n]
    return jnp.where(k == 0, a, b), jnp.where(k == 0, b, a)


HB = 2


def _own_body(ids, qm, qs, km, ks, vm, vs, acc_ref, top_ref):
    k = ids[1]
    tasks = []
    for n in range(HB):
        q, kk, v = _pair(k, qm, qs, n), _pair(k, km, ks, n), _pair(k, vm, vs, n)
        tasks += [(q[0], kk[0], v[0], True), (q[1], kk[0], v[0], False), (q[1], kk[1], v[1], True)]
    done = _tasks(tasks)
    for n in range(HB):
        a, b, c = done[3 * n : 3 * n + 3]
        for j, (acc, top) in enumerate((a, _merge([b, c]))):
            acc_ref[n, j], top_ref[n, j] = acc, top


def _o0_body(ids, qm, qs, km, ks, vm, vs, q0, k0, v0, acc_in, top_in, acc_ref, top_ref, seen_ref):
    c, k = ids[0], ids[1]
    late = c == 0
    tasks = []
    for n in range(HB):
        q, kk, v = _pair(k, qm, qs, n), _pair(k, km, ks, n), _pair(k, vm, vs, n)
        tasks += [(q0[n], k0[n], v0[n], True)]
        for j in range(2):
            tasks += [(jnp.where(late, q0[n], q[j]), jnp.where(late, kk[j], k0[n]), jnp.where(late, v[j], v0[n]), False)]
    done = _tasks(tasks)
    for n in range(HB):
        d, *f = done[3 * n : 3 * n + 3]
        seen_ref[:, n * HEAD : (n + 1) * HEAD] = _ended(_merge([d, _if(late, f[0]), _if(late, f[1])]))
        for j in range(2):
            acc_ref[n, j], top_ref[n, j] = _merge([(acc_in[n, j], top_in[n, j]), _if(c == 1, f[j])])


def _o1_body(ids, qm, qs, km, ks, vm, vs, q0, k0, v0, q1, k1, v1, acc_in, top_in, seen_in, *outs):
    own_m, own_s, oth_m, oth_s = outs
    c, k = ids[0], ids[1]
    late = c == 0
    tasks = []
    for n in range(HB):
        q, kk, v = _pair(k, qm, qs, n), _pair(k, km, ks, n), _pair(k, vm, vs, n)
        tasks += [(q1[n], k1[n], v1[n], True), (q1[n], k0[n], v0[n], False)]
        for j in range(2):
            tasks += [(jnp.where(late, q1[n], q[j]), jnp.where(late, kk[j], k1[n]), jnp.where(late, v[j], v1[n]), False)]
    done = _tasks(tasks)

    def put(m, s, j, n, o):
        cols = slice(n * HEAD, (n + 1) * HEAD)
        half = BLOCK // 2
        lo, hi = o[:half], o[half:]
        for refs, rows, e in ((m, jnp.where(k == 0, lo, hi), k if j == 0 else 1 - k), (s, jnp.where(k == 0, hi, lo), 1 - k if j == 0 else k)):
            for p in range(2):
                refs[p, e, :, cols] = rows[p * 128 : (p + 1) * 128]

    for n in range(HB):
        d, z, *f = done[4 * n : 4 * n + 4]
        put(oth_m, oth_s, 0, n, seen_in[:, n * HEAD : (n + 1) * HEAD])
        put(oth_m, oth_s, 1, n, _ended(_merge([d, z, _if(late, f[0]), _if(late, f[1])])))
        for j in range(2):
            put(own_m, own_s, j, n, _ended(_merge([(acc_in[n, j], top_in[n, j]), _if(c == 1, f[j])])))


def _attend(body, ids, qkvs, state, seen, outs, tasks, name):
    one = lambda i, ids: (i, 0, 0)
    qk, v = (HB, BLOCK, HEAD), (HB, HEAD, BLOCK)
    ins = []
    if len(qkvs) >= 2:
        for i in range(3):
            ins += [(t[i], v if i == 2 else qk, one) for t in qkvs[:2]]
    for t in qkvs[2:]:
        ins += [(t[0], qk, one), (t[1], qk, one), (t[2], v, one)]
    if state is not None:
        ins += [(state[0], (HB, 2, HEAD + 8, BLOCK), lambda i, ids: (i, 0, 0, 0)), (state[1], (HB, 2, 1, BLOCK), lambda i, ids: (i, 0, 0, 0))]
    if seen is not None:
        ins += [(seen, (BLOCK, HB * HEAD), lambda i, ids: (0, i))]
    n = HEADS * tasks * BLOCK * BLOCK
    return _call(body, ids, (HEADS // HB,), ins, outs, flops=4 * n * HEAD * 2, exps=n, name=name)


STATE = [((HEADS, 2, HEAD + 8, BLOCK), F32, (HB, 2, HEAD + 8, BLOCK), lambda i, ids: (i, 0, 0, 0)),
         ((HEADS, 2, 1, BLOCK), F32, (HB, 2, 1, BLOCK), lambda i, ids: (i, 0, 0, 0))]
SEEN = ((BLOCK, HEADS * HEAD), BF16, (BLOCK, HB * HEAD), lambda i, ids: (0, i))
PIECE = ((2, 2, 128, HEADS * HEAD), BF16, (2, 2, 128, HB * HEAD), lambda i, ids: (0, 0, 0, i))


R = 128
M = 2 * R
TILE = 256
OTH, OWN = 0, 1


def _mlp_body(gain, own_m, own_s, oth_m, oth_s, x, xs, r0, r1, *refs):
    wo, (wg, wu, wd, y), scratch = refs[:10], refs[10:14], refs[14:]
    S, WO, X, HS, WG, WU, WD, B, H, SA, SF, SN, AW, FAR, NEAR, lsem, ssem, rsem = scratch
    t, g = lax.axis_index("tp"), lax.axis_index("dp")
    k = lax.rem(t, 2)
    sib, cross, diag = t + 1 - 2 * k, lax.rem(t + 2, 4), 3 - t
    used = [0, 0]

    def local(src, dst):
        used[0] += 1
        copy = pltpu.make_async_copy(src, dst, lsem.at[used[0] - 1])
        copy.start()
        return copy

    def remote(src, dst, to):
        i = used[1]
        used[1] += 1
        copy = pltpu.make_async_remote_copy(src, dst, ssem.at[i], rsem.at[i], device_id={"tp": to}, device_id_type=pl.DeviceIdType.MESH)
        copy.start()
        return copy

    barrier = pltpu.get_barrier_semaphore()
    for d in (sib, cross, diag):
        pl.semaphore_signal(barrier, inc=1, device_id={"tp": d}, device_id_type=pl.DeviceIdType.MESH)

    mine = pl.ds(pl.multiple_of(512 * t, 512), 512)
    here = {}
    for pair, src in ((OTH, oth_m), (OWN, own_m)):
        for p in range(2):
            here[pair, p] = [local(src.at[p], S.at[pair, p, :, :, mine])]
    w = [local(wo[0], WO.at[mine]), local(wo[1], WO.at[pl.ds(pl.multiple_of(512 * sib, 512), 512)])]
    for who, d in enumerate((cross, diag)):
        for what in range(4):
            half = g if what < 2 else 1 - g
            at = pl.multiple_of(512 * d + 256 * half + 128 * (what % 2), 128)
            w.append(local(wo[2 + 4 * who + what], WO.at[pl.ds(at, 128)]))
    for p in range(2):
        rows = pl.ds(pl.multiple_of(256 * k + R * p, R), R)
        part = pl.ds(R * p, R)
        here[OTH, p] += [local(r0.at[part], X.at[OTH, p, k]), local(r1.at[part], X.at[OTH, p, 1 - k])]
        here[OWN, p] += [local(x.at[rows], X.at[OWN, p, 0]), local(xs.at[rows], X.at[OWN, p, 1])]

    pl.semaphore_wait(barrier, 3)
    sends = []
    there = {}
    for pair, (to_sib, to_cross, to_diag) in ((OTH, (oth_s, own_m, own_s)), (OWN, (own_s, oth_m, oth_s))):
        for p in range(2):
            there[pair, p] = [remote(src.at[p], S.at[pair, p, :, :, mine], d) for src, d in ((to_sib, sib), (to_cross, cross), (to_diag, diag))]
            sends += there[pair, p]
    mlp_w = [local(wg, WG), local(wu, WU), local(wd, WD)]

    def h_of(pair, p):
        for copy in here[pair, p]:
            copy.wait()
        for copy in there[pair, p]:
            copy.wait_recv()
        seen = S[pair, p].reshape(M, 2048)
        for n in range(0, 2048, TILE):
            cols = slice(n, n + TILE)
            h = X[pair, p, :, :, cols].reshape(M, TILE).astype(F32) + _dot(seen, WO[:, cols])
            X[pair, p, :, :, cols] = h.astype(BF16).reshape(2, R, TILE)
        copy = remote(X.at[pair, p], HS.at[pair, p], sib)
        sends.append(copy)
        return copy

    def mlp(pair, p, e, arrived, out, before=()):
        if arrived is not None:
            arrived.wait_recv()
        B[:R, :] = _normed(X[pair, p, e], gain[...])
        B[R:, :] = _normed(HS[pair, p, 1 - e], gain[...])
        b = B[...]
        for n in range(0, 2048, TILE):
            cols = slice(n, n + TILE)
            gate, up = _dot(b, WG[:, cols]), _dot(b, WU[:, cols])
            H[:, cols] = (gate * jax.nn.sigmoid(gate) * up).astype(BF16)
        for copy in before:
            copy.wait_recv()
        hidden = H[...]
        for n in range(0, 2048, TILE):
            cols = slice(n, n + TILE)
            out(cols, _dot(hidden, WD[:, cols]))

    def keep(ref, p, cols, term):
        ref[p, :, cols] = term.astype(BF16)

    def swapped(ref, p, cols):
        return jnp.concatenate([ref[p, R:, cols], ref[p, :R, cols]], 0).astype(F32)

    def to_far(p, cols, term):
        SF[p, :, cols] = (term + swapped(AW, p, cols)).astype(BF16)

    def to_y(p, cols, term):
        h = jnp.concatenate([X[OWN, p, 0, :, cols], HS[OWN, p, 1, :, cols]], 0).astype(F32)
        SA[p, :, cols] = (h + term + swapped(NEAR, p, cols) + FAR[p, :, cols].astype(F32)).astype(BF16)

    for copy in w:
        copy.wait()
    hs = [h_of(OTH, p) for p in range(2)]
    for copy in mlp_w:
        copy.wait()
    away = []
    for p in range(2):
        mlp(OTH, p, 1, hs[p], functools.partial(keep, SA, p))
        away.append(remote(SA.at[p], AW.at[p], sib))
    far = []
    for p in range(2):
        mlp(OTH, p, 0, None, functools.partial(to_far, p), [away[p]])
        far.append(remote(SF.at[p], FAR.at[p], cross))
    hs = [h_of(OWN, p) for p in range(2)]
    near = []
    for p in range(2):
        mlp(OWN, p, 1, hs[p], functools.partial(keep, SN, p))
        near.append(remote(SN.at[p], NEAR.at[p], sib))
    for copy in away:
        copy.wait_send()
    done = []
    for p in range(2):
        mlp(OWN, p, 0, None, functools.partial(to_y, p), [near[p], far[p]])
        for e, half in enumerate((k, 1 - k)):
            rows = pl.ds(pl.multiple_of(256 * half + R * p, R), R)
            done.append(local(SA.at[p, pl.ds(R * e, R)], y.at[rows]))
    for copy in [*sends, *far, *near]:
        copy.wait_send()
    for copy in done:
        copy.wait()


def _mlp(gain, seen, x, wo, weights):
    ins = [gain, *seen, *x, *wo, *weights]
    vmem, hbm = pl.BlockSpec(memory_space=pltpu.VMEM), pl.BlockSpec(memory_space=pl.ANY)
    big = pltpu.VMEM((2, M, 2048), BF16)
    pairs = pltpu.VMEM((2, 2, 2, R, 2048), BF16)
    weight = pltpu.VMEM((2048, 2048), BF16)
    block = pltpu.VMEM((M, 2048), BF16)
    return pl.pallas_call(
        _mlp_body,
        in_specs=[vmem] + [hbm] * (len(ins) - 1),
        out_specs=hbm,
        out_shape=jax.ShapeDtypeStruct((512, 2048), BF16),
        scratch_shapes=[pairs, weight, pairs, pairs, weight, weight, weight, block, block, *[big] * 6,
                        pltpu.SemaphoreType.DMA((40,)), pltpu.SemaphoreType.DMA((24,)), pltpu.SemaphoreType.DMA((24,))],
        compiler_params=pltpu.CompilerParams(collective_id=1, has_side_effects=True, vmem_limit_bytes=67_043_328),
        cost_estimate=pl.CostEstimate(flops=2 * 2048**3 * 3, transcendentals=2048**2, bytes_accessed=2**26),
        name="mlp",
    )(*ins)


def solution(mesh):
    def pp(t, perm):
        return lax.ppermute(t, "tp", perm)

    def over(t):
        return lax.ppermute(t, "dp", [(0, 1), (1, 0)])

    def step(x, gain_a, wq, wk, wv, wo, gain_m, w_gate, w_up, w_down):
        t, g = lax.axis_index("tp"), lax.axis_index("dp")
        c, k = t // 2, t % 2
        ids = jnp.stack([c, k, g]).astype(jnp.int32)
        gain_a, gain_m = gain_a[None], gain_m[None]
        tab = jnp.asarray(_table())
        even = k == 0

        lo, hi = x[:256], x[256:]
        xs_hi = pp(hi, SIB)
        xs = pp(x, SIB)
        r0 = pp(jnp.where(even, lo, xs_hi), CROSS)
        r1 = pp(jnp.where(even, xs[:256], hi), CROSS)

        wa = lax.dynamic_slice_in_dim(wo, 256 * g, 128, 0)
        wb = lax.dynamic_slice_in_dim(wo, 256 * g + 128, 128, 0)
        (wa, wb), _ = lax.optimization_barrier(((wa, wb), r1))
        wa, wb = pp(wa, CROSS), pp(wb, CROSS)
        ya, yb = over(wa), over(wb)
        cross_wo = [wa, wb, ya, yb]
        wos = [wo, pp(wo, SIB), *cross_wo, *[pp(w, SIB) for w in cross_wo]]

        weights = (gain_a, wq, wk, wv, tab)
        me = _qkv(ids, [x], lambda i: 2 * i[0] + i[1], *weights)
        sib = _qkv(ids, [xs], lambda i: 2 * i[0] + 1 - i[1], *weights)
        state = _attend(_own_body, ids, [me, sib], None, None, STATE, 3, "attn_own")
        o0 = _qkv(ids, [r0, pp(r0, SIB)], lambda i: 2 - 2 * i[0], *weights)
        *state, seen0 = _attend(_o0_body, ids, [me, sib, o0], state, None, [*STATE, SEEN], 3, "attn_o0")
        o1 = _qkv(ids, [r1, pp(r1, SIB)], lambda i: 3 - 2 * i[0], *weights)
        seen = _attend(_o1_body, ids, [me, sib, o0, o1], state, seen0, [PIECE] * 4, 4, "attn_o1")
        return _mlp(gain_m, seen, (x, xs, r0, r1), wos, (w_gate, w_up, w_down))

    tokens, columns, rows_of = P(("dp", "tp"), None), P(None, "tp"), P("tp", None)
    return jax.shard_map(
        step,
        mesh=mesh,
        in_specs=(tokens, P(None), columns, columns, columns, rows_of, P(None), columns, columns, rows_of),
        out_specs=tokens,
        check_vma=False,
    )
```

```python
import functools

import jax
import jax.numpy as jnp
import numpy as np
from jax import lax
from jax.experimental import pallas as pl
from jax.experimental.pallas import tpu as pltpu
from jax.sharding import PartitionSpec as P

HEAD = 128
HEADS = 4
BLOCK = 512
THETA = 10000
NEG = -1e30
HIDDEN = 2 * NEG
LOG2E = 1.4426950408889634
F32, BF16 = jnp.float32, jnp.bfloat16


def _dot(a, b, ca=1, cb=0):
    return lax.dot_general(a, b, (((ca,), (cb,)), ((), ())), preferred_element_type=F32)


def _normed(x, gain):
    wide = x.astype(F32)
    scale = lax.rsqrt(jnp.mean(wide * wide, -1, keepdims=True) + 1e-6)
    return (wide * scale * gain.astype(F32)).astype(BF16)


def _table():
    half = HEAD // 2
    rate = np.float32(THETA) ** (-np.arange(half, dtype=np.float32) / np.float32(half))
    angle = np.arange(2048, dtype=np.float32)[:, None] * rate.astype(np.float32)
    return np.concatenate([np.cos(angle), np.sin(angle)], 1).astype(np.float32)


E = HEAD**-0.5 * LOG2E


def _scores(q, k, diagonal):
    s = _dot(k, q, 1, 1)
    if diagonal:
        s = jnp.where(lax.broadcasted_iota(jnp.int32, s.shape, 1) >= lax.broadcasted_iota(jnp.int32, s.shape, 0), s, HIDDEN)
    return s


def _tasks(tasks):
    scores = [_scores(q, k, d) for q, k, _, d in tasks]
    out = []
    for (_, _, v, _), s in zip(tasks, scores):
        top = s.max(axis=0, keepdims=True)
        p = jnp.exp2((s - top) * E).astype(BF16)
        out.append((p, top))
    ones = jnp.ones((8, BLOCK), BF16)
    return [(_dot(jnp.concatenate([v, ones], 0), p), top) for (_, _, v, _), (p, top) in zip(tasks, out)]


def _merge(parts):
    top = functools.reduce(jnp.maximum, [t for _, t in parts])
    return sum(a * jnp.exp2((t - top) * E) for a, t in parts), top


def _if(ok, part):
    return part[0], jnp.where(ok, part[1], NEG)


def _ended(part):
    acc = part[0]
    return (acc[:HEAD] * (1 / acc[HEAD : HEAD + 1])).T.astype(BF16)


HB = 2
R = 128


def _mesh_copy(src, dst, ssem, rsem, axis, to):
    return pltpu.make_async_remote_copy(src, dst, ssem, rsem, device_id={axis: to}, device_id_type=pl.DeviceIdType.MESH)


def _greet(peers):
    barrier = pltpu.get_barrier_semaphore()
    for axis, d in peers:
        pl.semaphore_signal(barrier, inc=1, device_id={axis: d}, device_id_type=pl.DeviceIdType.MESH)
    return barrier


def _attn_body(gain, x, wq, wk, wv, wo, tab, own_m, own_s, oth_m, oth_s, xres, wof, X, W, T, A, QS, KS, VS, ACC, TOP, lsem, ssem, rsem):
    t, g = lax.axis_index("tp"), lax.axis_index("dp")
    c, k = lax.div(t, 2), lax.rem(t, 2)
    sib, cross = t + 1 - 2 * k, lax.rem(t + 2, 4)
    used = [0, 0]

    def local(src, dst):
        used[0] += 1
        copy = pltpu.make_async_copy(src, dst, lsem.at[used[0] - 1])
        copy.start()
        return copy

    def remote(src, dst, to, axis="tp", start=True):
        i = used[1]
        used[1] += 1
        copy = _mesh_copy(src, dst, ssem.at[i], rsem.at[i], axis, to)
        if start:
            copy.start()
        return copy

    barrier = _greet((("tp", sib), ("tp", cross), ("dp", 1 - g)))
    got_x = local(x, X.at[k])
    got_w = [local(w, W.at[i]) for i, w in enumerate((wq, wk, wv))]
    got_t = local(tab, T)
    pl.semaphore_wait(barrier, 3)

    hi = remote(x.at[pl.ds(256, 256)], X.at[k, pl.ds(256, 256)], sib)
    lo = remote(x.at[pl.ds(0, 256)], X.at[k, pl.ds(0, 256)], sib)
    rows = [pl.ds(pl.multiple_of(256 * k + R * p, R), R) for p in range(2)]
    first = [remote(X.at[0, rows[p]], X.at[2, rows[p]], cross, start=False) for p in range(2)]

    @pl.when(k == 0)
    def _():
        for p in range(2):
            _mesh_copy(x.at[pl.ds(R * p, R)], X.at[2, rows[p]], ssem.at[2 + p], rsem.at[2 + p], "tp", cross).start()

    hi.wait_recv()

    @pl.when(k == 1)
    def _():
        for p in range(2):
            first[p].start()

    got_x.wait()
    lo.wait_recv()
    second = [remote(X.at[1, rows[p]], X.at[3, rows[p]], cross) for p in range(2)]
    mine = pl.multiple_of(512 * t, 512)
    theirs = pl.multiple_of(512 * cross, 512)
    part = [256 * g + R * p for p in range(2)]
    other = 256 * (1 - g)
    wos = [remote(wo.at[pl.ds(pl.multiple_of(part[p], R), R)], wof.at[pl.ds(pl.multiple_of(mine + part[p], R), R)], cross) for p in range(2)]
    whole = remote(wo, wof.at[pl.ds(mine, 512)], sib)
    sent = [hi, lo, *first, *second, *wos, whole]
    kept = []

    def keep(pair, e, block):
        for p in range(2):
            kept.append(local(X.at[block, rows[p]], xres.at[pair, p, e]))

    def qkv(block, place):
        A[...] = _normed(X[block], gain[...])
        tt = T[pl.ds(pl.multiple_of(place * BLOCK, BLOCK), BLOCK), :]
        flip = pltpu.roll(tt, HEAD // 2, 1)
        left = lax.broadcasted_iota(jnp.int32, tt.shape, 1) < HEAD // 2
        cos, sin = jnp.where(left, tt, flip), jnp.where(left, -flip, tt)
        a = A[...]
        for h in range(0, HEADS, 2):
            cols = slice(h * HEAD, (h + 2) * HEAD)
            for i, out in enumerate((QS, KS)):
                y = _dot(a, W[i, :, cols]).astype(BF16).astype(F32)
                for n in range(2):
                    z = y[:, n * HEAD : (n + 1) * HEAD]
                    out[block, h + n] = (z * cos + pltpu.roll(z, HEAD // 2, 1) * sin).astype(BF16)
            v = _dot(a, W[2, :, cols]).astype(BF16)
            for n in range(2):
                VS[block, h + n] = v[:, n * HEAD : (n + 1) * HEAD].T

    late = c == 0

    def task(n, q, kv, diagonal=False):
        return QS[q, n], KS[kv, n], VS[kv, n], diagonal

    def either(n, j, o):
        q, kv = jnp.where(late, o, j), jnp.where(late, j, o)
        return task(n, q, kv)

    def put(m, s, j, n, o):
        cols = pl.ds(pl.multiple_of(n * HEAD, HEAD), HEAD)
        half = BLOCK // 2
        lo, hi = o[:half], o[half:]
        for ref, v, e in ((m, jnp.where(k == 0, lo, hi), k if j == 0 else 1 - k), (s, jnp.where(k == 0, hi, lo), 1 - k if j == 0 else k)):
            for p in range(2):
                ref[p, e, :, cols] = v[p * R : (p + 1) * R]

    def own(i, _):
        heads = [HB * i + n for n in range(HB)]
        done = _tasks([u for n in heads for u in (task(n, 0, 0, True), task(n, 1, 0), task(n, 1, 1, True))])
        for at, n in enumerate(heads):
            a, *b = done[3 * at : 3 * at + 3]
            for j, (acc, top) in enumerate((a, _merge(b))):
                ACC[n, j], TOP[n, j] = acc, top

    def third(i, _):
        heads = [HB * i + n for n in range(HB)]
        done = _tasks([u for n in heads for u in (task(n, 2, 2, True), either(n, 0, 2), either(n, 1, 2))])
        for at, n in enumerate(heads):
            d, *f = done[3 * at : 3 * at + 3]
            put(oth_m, oth_s, 0, n, _ended(_merge([d, _if(late, f[0]), _if(late, f[1])])))
            for j in range(2):
                ACC[n, j], TOP[n, j] = _merge([(ACC[n, j], TOP[n, j]), _if(c == 1, f[j])])

    def fourth(i, _):
        heads = [HB * i + n for n in range(HB)]
        done = _tasks([u for n in heads for u in (task(n, 3, 3, True), task(n, 3, 2), either(n, 0, 3), either(n, 1, 3))])
        for at, n in enumerate(heads):
            d, z, *f = done[4 * at : 4 * at + 4]
            put(oth_m, oth_s, 1, n, _ended(_merge([d, z, _if(late, f[0]), _if(late, f[1])])))
            for j in range(2):
                put(own_m, own_s, j, n, _ended(_merge([(ACC[n, j], TOP[n, j]), _if(c == 1, f[j])])))

    def arrive(copies, block):
        on = []
        for p, copy in enumerate(copies):
            copy.wait_recv()
            on.append(remote(X.at[block, rows[p]], X.at[block, rows[p]], sib))
        sent.extend(on)
        for copy in on:
            copy.wait_recv()

    for copy in got_w:
        copy.wait()
    got_t.wait()
    qkv(k, 2 * c + k)
    qkv(1 - k, 2 * c + 1 - k)
    keep(1, 0, k)
    keep(1, 1, 1 - k)
    lax.fori_loop(0, HEADS // HB, own, None)
    arrive(first, 2)
    qkv(2, 2 - 2 * c)
    lax.fori_loop(0, HEADS // HB, third, None)
    arrive(second, 3)
    qkv(3, 3 - 2 * c)
    keep(0, k, 2)
    keep(0, 1 - k, 3)
    fourth(0, None)
    wos[0].wait_recv()
    at = pl.ds(pl.multiple_of(theirs + part[0], R), R)
    on = remote(wof.at[at], wof.at[at], 1 - g, "dp")
    sent += [on, remote(wof.at[at], wof.at[at], sib)]
    whole.wait_recv()
    fourth(1, None)
    on.wait_recv()
    at = pl.ds(pl.multiple_of(theirs + other, R), R)
    sent.append(remote(wof.at[at], wof.at[at], sib))
    for copy in (sent[-2], sent[-1], wos[1]):
        copy.wait_recv()
    for copy in sent:
        copy.wait_send()
    for copy in kept:
        copy.wait()


def _attn(gain, x, wq, wk, wv, wo, tab):
    vmem, hbm = pl.BlockSpec(memory_space=pltpu.VMEM), pl.BlockSpec(memory_space=pl.ANY)
    piece = jax.ShapeDtypeStruct((2, 2, R, HEADS * HEAD), BF16)
    heads = pltpu.VMEM((4, HEADS, BLOCK, HEAD), BF16)
    return pl.pallas_call(
        _attn_body,
        in_specs=[vmem] + [hbm] * 6,
        out_specs=[vmem] * 4 + [hbm] * 2,
        out_shape=[piece] * 4 + [jax.ShapeDtypeStruct((2, 2, 2, R, 2048), BF16), jax.ShapeDtypeStruct((2048, 2048), BF16)],
        scratch_shapes=[pltpu.VMEM((4, BLOCK, 2048), BF16), pltpu.VMEM((3, 2048, BLOCK), BF16), pltpu.VMEM((2048, HEAD), F32),
                        pltpu.VMEM((BLOCK, 2048), BF16), heads, heads, pltpu.VMEM((4, HEADS, HEAD, BLOCK), BF16),
                        pltpu.VMEM((HEADS, 2, HEAD + 8, BLOCK), F32), pltpu.VMEM((HEADS, 2, 1, BLOCK), F32),
                        pltpu.SemaphoreType.DMA((16,)), pltpu.SemaphoreType.DMA((18,)), pltpu.SemaphoreType.DMA((18,))],
        compiler_params=pltpu.CompilerParams(collective_id=2, has_side_effects=True, vmem_limit_bytes=60 * 2**20),
        cost_estimate=pl.CostEstimate(flops=2 * 2048 * 2048 * 1536, transcendentals=4 * 2**21, bytes_accessed=2**25),
        name="attn",
    )(gain, x, wq, wk, wv, wo, tab)


M = 2 * R
TILE = 256
OTH, OWN = 0, 1


def _mlp_body(gain, own_m, own_s, oth_m, oth_s, xres, wof, wo, wg, wu, wd, y, *scratch):
    S, WO, X, HS, WG, WU, WD, B, H, SA, SF, SN, AW, FAR, NEAR, lsem, ssem, rsem = scratch
    t, g = lax.axis_index("tp"), lax.axis_index("dp")
    k = lax.rem(t, 2)
    sib, cross, diag = t + 1 - 2 * k, lax.rem(t + 2, 4), 3 - t
    used = [0, 0]

    def local(src, dst):
        used[0] += 1
        copy = pltpu.make_async_copy(src, dst, lsem.at[used[0] - 1])
        copy.start()
        return copy

    def remote(src, dst, to, axis="tp"):
        i = used[1]
        used[1] += 1
        copy = _mesh_copy(src, dst, ssem.at[i], rsem.at[i], axis, to)
        copy.start()
        return copy

    barrier = _greet((("tp", sib), ("tp", cross), ("tp", diag), ("dp", 1 - g)))

    mine = pl.ds(pl.multiple_of(512 * t, 512), 512)
    here = {}
    for pair, src in ((OTH, oth_m), (OWN, own_m)):
        for p in range(2):
            here[pair, p] = [local(src.at[p], S.at[pair, p, :, :, mine])]
    def wo_rows(who, half, p, n=1):
        return pl.ds(pl.multiple_of(512 * who + 256 * half + R * p, R), n * R)

    w = [local(wo, WO.at[mine]), local(wof.at[wo_rows(sib, 0, 0, 4)], WO.at[wo_rows(sib, 0, 0, 4)])]
    for who, half, p in ((cross, g, 0), (cross, 1 - g, 0), (cross, g, 1), (diag, g, 0), (diag, 1 - g, 0)):
        w.append(local(wof.at[wo_rows(who, half, p)], WO.at[wo_rows(who, half, p)]))
    for pair in range(2):
        for p in range(2):
            here[pair, p].append(local(xres.at[pair, p], X.at[pair, p]))

    pl.semaphore_wait(barrier, 4)
    late = wo_rows(cross, g, 1)
    over = remote(wof.at[late], WO.at[late], 1 - g, "dp")
    across = remote(wof.at[late], WO.at[late], sib)
    sends = [over, across]
    there = {}
    for pair, (to_sib, to_cross, to_diag) in ((OTH, (oth_s, own_m, own_s)), (OWN, (own_s, oth_m, oth_s))):
        for p in range(2):
            there[pair, p] = [remote(src.at[p], S.at[pair, p, :, :, mine], d) for src, d in ((to_sib, sib), (to_cross, cross), (to_diag, diag))]
            sends += there[pair, p]
    mlp_w = [local(wg, WG), local(wu, WU), local(wd, WD)]

    def h_of(pair, p):
        for copy in here[pair, p]:
            copy.wait()
        for copy in there[pair, p]:
            copy.wait_recv()
        seen = S[pair, p].reshape(M, 2048)
        for n in range(0, 2048, TILE):
            cols = slice(n, n + TILE)
            h = X[pair, p, :, :, cols].reshape(M, TILE).astype(F32) + _dot(seen, WO[:, cols])
            X[pair, p, :, :, cols] = h.astype(BF16).reshape(2, R, TILE)
        copy = remote(X.at[pair, p], HS.at[pair, p], sib)
        sends.append(copy)
        return copy

    def mlp(pair, p, e, arrived, out, before=()):
        if arrived is not None:
            arrived.wait_recv()
        B[:R, :] = _normed(X[pair, p, e], gain[...])
        B[R:, :] = _normed(HS[pair, p, 1 - e], gain[...])
        b = B[...]
        for n in range(0, 2048, TILE):
            cols = slice(n, n + TILE)
            gate, up = _dot(b, WG[:, cols]), _dot(b, WU[:, cols])
            H[:, cols] = (gate * jax.nn.sigmoid(gate) * up).astype(BF16)
        for copy in before:
            copy.wait_recv()
        hidden = H[...]
        for n in range(0, 2048, TILE):
            cols = slice(n, n + TILE)
            out(cols, _dot(hidden, WD[:, cols]))

    def keep(ref, p, cols, term):
        ref[p, :, cols] = term.astype(BF16)

    def swapped(ref, p, cols):
        return jnp.concatenate([ref[p, R:, cols], ref[p, :R, cols]], 0).astype(F32)

    def to_far(p, cols, term):
        SF[p, :, cols] = (term + swapped(AW, p, cols)).astype(BF16)

    def to_y(p, cols, term):
        h = jnp.concatenate([X[OWN, p, 0, :, cols], HS[OWN, p, 1, :, cols]], 0).astype(F32)
        SA[p, :, cols] = (h + term + swapped(NEAR, p, cols) + FAR[p, :, cols].astype(F32)).astype(BF16)

    for copy in w:
        copy.wait()
    over.wait_recv()
    late = wo_rows(cross, 1 - g, 1)
    sends.append(remote(WO.at[late], WO.at[late], sib))
    across.wait_recv()
    sends[-1].wait_recv()
    hs = [h_of(OTH, p) for p in range(2)]
    for copy in mlp_w:
        copy.wait()
    away = []
    for p in range(2):
        mlp(OTH, p, 1, hs[p], functools.partial(keep, SA, p))
        away.append(remote(SA.at[p], AW.at[p], sib))
    far = []
    for p in range(2):
        mlp(OTH, p, 0, None, functools.partial(to_far, p), [away[p]])
        far.append(remote(SF.at[p], FAR.at[p], cross))
    hs = [h_of(OWN, p) for p in range(2)]
    near = []
    for p in range(2):
        mlp(OWN, p, 1, hs[p], functools.partial(keep, SN, p))
        near.append(remote(SN.at[p], NEAR.at[p], sib))
    for copy in away:
        copy.wait_send()
    done = []
    for p in range(2):
        mlp(OWN, p, 0, None, functools.partial(to_y, p), [near[p], far[p]])
        for e, half in enumerate((k, 1 - k)):
            rows = pl.ds(pl.multiple_of(256 * half + R * p, R), R)
            done.append(local(SA.at[p, pl.ds(R * e, R)], y.at[rows]))
    for copy in [*sends, *far, *near]:
        copy.wait_send()
    for copy in done:
        copy.wait()


def _mlp(*ins):
    vmem, hbm = pl.BlockSpec(memory_space=pltpu.VMEM), pl.BlockSpec(memory_space=pl.ANY)
    big = pltpu.VMEM((2, M, 2048), BF16)
    pairs = pltpu.VMEM((2, 2, 2, R, 2048), BF16)
    weight = pltpu.VMEM((2048, 2048), BF16)
    block = pltpu.VMEM((M, 2048), BF16)
    return pl.pallas_call(
        _mlp_body,
        in_specs=[vmem] + [hbm] * (len(ins) - 1),
        out_specs=hbm,
        out_shape=jax.ShapeDtypeStruct((512, 2048), BF16),
        scratch_shapes=[pairs, weight, pairs, pairs, weight, weight, weight, block, block, *[big] * 6,
                        pltpu.SemaphoreType.DMA((32,)), pltpu.SemaphoreType.DMA((32,)), pltpu.SemaphoreType.DMA((32,))],
        compiler_params=pltpu.CompilerParams(collective_id=1, has_side_effects=True, vmem_limit_bytes=67_043_328),
        cost_estimate=pl.CostEstimate(flops=2 * 2048**3 * 3, transcendentals=2048**2, bytes_accessed=2**26),
        name="mlp",
    )(*ins)


def solution(mesh):
    def step(x, gain_a, wq, wk, wv, wo, gain_m, w_gate, w_up, w_down):
        *seen, xres, wof = _attn(gain_a[None], x, wq, wk, wv, wo, jnp.asarray(_table()))
        return _mlp(gain_m[None], *seen, xres, wof, wo, w_gate, w_up, w_down)

    tokens, columns, rows_of = P(("dp", "tp"), None), P(None, "tp"), P("tp", None)
    return jax.shard_map(
        step,
        mesh=mesh,
        in_specs=(tokens, P(None), columns, columns, columns, rows_of, P(None), columns, columns, rows_of),
        out_specs=tokens,
        check_vma=False,
    )
```

```python
import functools

import jax
import jax.numpy as jnp
import numpy as np
from jax import lax
from jax.experimental import pallas as pl
from jax.experimental.pallas import tpu as pltpu
from jax.sharding import PartitionSpec as P

HEAD = 128
HEADS = 4
BLOCK = 512
THETA = 10000
NEG = -1e30
HIDDEN = 2 * NEG
LOG2E = 1.4426950408889634
F32, BF16 = jnp.float32, jnp.bfloat16


def _dot(a, b, ca=1, cb=0):
    return lax.dot_general(a, b, (((ca,), (cb,)), ((), ())), preferred_element_type=F32)


def _normed(x, gain):
    wide = x.astype(F32)
    scale = lax.rsqrt(jnp.mean(wide * wide, -1, keepdims=True) + 1e-6)
    return (wide * scale * gain.astype(F32)).astype(BF16)


def _table():
    half = HEAD // 2
    rate = np.float32(THETA) ** (-np.arange(half, dtype=np.float32) / np.float32(half))
    angle = np.arange(2048, dtype=np.float32)[:, None] * rate.astype(np.float32)
    return np.concatenate([np.cos(angle), np.sin(angle)], 1).astype(np.float32)


E = HEAD**-0.5 * LOG2E


def _scores(q, k, diagonal):
    s = _dot(k, q, 1, 1)
    if diagonal:
        s = jnp.where(lax.broadcasted_iota(jnp.int32, s.shape, 1) >= lax.broadcasted_iota(jnp.int32, s.shape, 0), s, HIDDEN)
    return s


def _tasks(tasks):
    scores = [_scores(q, k, d) for q, k, _, d in tasks]
    out = []
    for (_, _, v, _), s in zip(tasks, scores):
        top = s.max(axis=0, keepdims=True)
        p = jnp.exp2((s - top) * E).astype(BF16)
        out.append((p, top))
    ones = jnp.ones((8, BLOCK), BF16)
    return [(_dot(jnp.concatenate([v, ones], 0), p), top) for (_, _, v, _), (p, top) in zip(tasks, out)]


def _merge(parts):
    top = functools.reduce(jnp.maximum, [t for _, t in parts])
    return sum(a * jnp.exp2((t - top) * E) for a, t in parts), top


def _if(ok, part):
    return part[0], jnp.where(ok, part[1], NEG)


def _ended(part):
    acc = part[0]
    return (acc[:HEAD] * (1 / acc[HEAD : HEAD + 1])).T.astype(BF16)


HB = 1
R = 128
M = 2 * R
TILE = 256
OTH, OWN = 0, 1


def _body(gain_a, gain_m, x, wq, wk, wv, wo, tab, wg, wu, wd, y, WO, WG, WU, WD, S, X, HS, B, H, SA, SF, AW, FAR, OS, TS, T, ACC, TOP,
          lsem, ssem, rsem):
    t, g = lax.axis_index("tp"), lax.axis_index("dp")
    c, k = lax.div(t, 2), lax.rem(t, 2)
    sib, cross, diag = t + 1 - 2 * k, lax.rem(t + 2, 4), 3 - t
    late = c == 0

    def rows(at, n):
        return pl.ds(pl.multiple_of(at, R), n)

    XB = lambda b, at=0, n=BLOCK: WD.at[rows(BLOCK * b + at, n)]
    WQKV = lambda i: WU.at[:, pl.ds(BLOCK * i, BLOCK)]
    KS = lambda b, n: WG.at[rows(BLOCK * b, BLOCK), rows(HEAD * n, HEAD)]
    QS = lambda b, n: WG.at[rows(BLOCK * b, BLOCK), rows(2 * BLOCK + HEAD * n, HEAD)]
    VS = lambda b, n: WG.at[rows(BLOCK * b + HEAD * n, HEAD), pl.ds(BLOCK, BLOCK)]

    def local(i, src, dst):
        return pltpu.make_async_copy(src, dst, lsem.at[i])

    def remote(i, src, dst, to, axis="tp"):
        return pltpu.make_async_remote_copy(
            src, dst, ssem.at[i], rsem.at[i], device_id={axis: to}, device_id_type=pl.DeviceIdType.MESH)

    barrier = pltpu.get_barrier_semaphore()
    for axis, d in (("tp", sib), ("tp", cross), ("tp", diag), ("dp", 1 - g)):
        pl.semaphore_signal(barrier, inc=1, device_id={axis: d}, device_id_type=pl.DeviceIdType.MESH)

    mine, theirs = 512 * t, 512 * cross
    own_rows = rows(mine, 512)
    cols = own_rows
    got_x = local(0, x, XB(k))
    got_w = [local(1 + i, w, WQKV(i)) for i, w in enumerate((wq, wk, wv))]
    got_t = local(4, tab, T)
    got_wo = local(5, wo, WO.at[own_rows])
    weights = [local(6 + i, w, to) for i, (w, to) in enumerate(((wg, WG), (wu, WU), (wd, WD)))]
    hi = remote(0, x.at[pl.ds(256, 256)], XB(k, 256, 256), sib)
    lo = remote(1, x.at[pl.ds(0, 256)], XB(k, 0, 256), sib)
    half = [256 * k + R * p for p in range(2)]
    first = [remote(2 + p, XB(0, half[p], R), XB(2, half[p], R), cross) for p in range(2)]
    direct = [remote(2 + p, x.at[pl.ds(R * p, R)], XB(2, half[p], R), cross) for p in range(2)]
    second = [remote(4 + p, XB(1, half[p], R), XB(3, half[p], R), cross) for p in range(2)]
    first_on = [remote(9 + p, XB(2, half[p], R), XB(2, half[p], R), sib) for p in range(2)]
    second_on = [remote(11 + p, XB(3, half[p], R), XB(3, half[p], R), sib) for p in range(2)]
    part = [256 * g + R * p for p in range(2)]
    wos = [remote(6 + p, wo.at[rows(part[p], R)], WO.at[rows(mine + part[p], R)], cross) for p in range(2)]
    whole = remote(8, wo, WO.at[own_rows], sib)
    came = [WO.at[rows(theirs + part[p], R)] for p in range(2)]
    lent = [WO.at[rows(theirs + 256 * (1 - g) + R * p, R)] for p in range(2)]
    over = [remote(13 + p, came[p], came[p], 1 - g, "dp") for p in range(2)]
    came_on = [remote(15 + p, came[p], came[p], sib) for p in range(2)]
    lent_on = [remote(17 + p, lent[p], lent[p], sib) for p in range(2)]

    def seen(pair, p):
        i = 19 + 6 * pair + 3 * p
        to = S.at[pair, p, :, :, cols]
        return [remote(i, (TS if pair == OTH else OS).at[p], to, sib), remote(i + 1, S.at[1 - pair, p, :, :, cols], to, cross),
                remote(i + 2, (OS if pair == OTH else TS).at[p], to, diag)]

    def seen_here(pair, p):
        i = 19 + 6 * pair + 3 * p
        return [remote(i + n, OS.at[p], S.at[pair, p, :, :, cols], sib) for n in range(3)]

    def hs(pair, p):
        return remote(31 + 2 * pair + p, X.at[pair, p], HS.at[pair, p], sib)

    def away(p):
        return remote(35 + p, SA.at[p], AW.at[p], sib)

    def far(p):
        return remote(37 + p, SF.at[p], FAR.at[p], cross)

    def near(p):
        return [remote(39 + 2 * p + j, SA.at[p, pl.ds(j * R, R)], S.at[OTH, p, j], sib) for j in range(2)]

    def result(p, e):
        return local(9 + 2 * p + e, AW.at[p, pl.ds(R * e, R)], y.at[rows(256 * (k if e == 0 else 1 - k) + R * p, R)])

    for copy in (got_x, *got_w, got_t, got_wo):
        copy.start()
    pl.semaphore_wait(barrier, 4)
    hi.start()
    lo.start()

    @pl.when(k == 0)
    def _():
        for copy in direct:
            copy.start()

    hi.wait_recv()

    @pl.when(k == 1)
    def _():
        for copy in first:
            copy.start()

    got_x.wait()
    lo.wait_recv()
    for copy in (*second, *wos, whole):
        copy.start()

    def qkv(block, place):
        a = _normed(XB(block)[...], gain_a[...][None])
        SA[0] = a[:M]
        SA[1] = a[M:]
        tt = T[rows(place * BLOCK, BLOCK), :]
        flip = pltpu.roll(tt, HEAD // 2, 1)
        left = lax.broadcasted_iota(jnp.int32, tt.shape, 1) < HEAD // 2
        cos, sin = jnp.where(left, tt, flip), jnp.where(left, -flip, tt)
        a = SA[...].reshape(BLOCK, 2048)
        for h in range(0, HEADS, 2):
            for i, out in enumerate((QS, KS)):
                z2 = _dot(a, WU[:, BLOCK * i + HEAD * h : BLOCK * i + HEAD * (h + 2)]).astype(BF16).astype(F32)
                for n in range(2):
                    z = z2[:, n * HEAD : (n + 1) * HEAD]
                    out(block, h + n)[...] = (z * cos + pltpu.roll(z, HEAD // 2, 1) * sin).astype(BF16)
            v = _dot(a, WU[:, 2 * BLOCK + HEAD * h : 2 * BLOCK + HEAD * (h + 2)]).astype(BF16)
            for n in range(2):
                VS(block, h + n)[...] = v[:, n * HEAD : (n + 1) * HEAD].T

    def task(n, q, kv, diagonal=False):
        return QS(q, n)[...], KS(kv, n)[...], VS(kv, n)[...], diagonal

    def either(n, j, o):
        return task(n, jnp.where(late, o, j), jnp.where(late, j, o))

    def put(pair, j, n, o):
        lo, hi = o[: BLOCK // 2], o[BLOCK // 2 :]
        e = k if j == 0 else 1 - k
        m, s = jnp.where(k == 0, lo, hi), jnp.where(k == 0, hi, lo)
        for p in range(2):
            S[pair, p, e, :, rows(mine + HEAD * n, HEAD)] = m[p * R : (p + 1) * R]
            (OS if pair == OWN else TS)[p, 1 - e, :, rows(HEAD * n, HEAD)] = s[p * R : (p + 1) * R]

    def second_phase(n, _):
        a, *b = _tasks([task(n, 0, 0, True), task(n, 1, 0), task(n, 1, 1, True)])
        for j, (acc, top) in enumerate((a, _merge(b))):
            ACC[n, j], TOP[n, j] = acc, top

    def third_phase(n, _):
        d, *f = _tasks([task(n, 2, 2, True), either(n, 0, 2), either(n, 1, 2)])
        put(OTH, 0, n, _ended(_merge([d, _if(late, f[0]), _if(late, f[1])])))
        for j in range(2):
            ACC[n, j], TOP[n, j] = _merge([(ACC[n, j], TOP[n, j]), _if(c == 1, f[j])])

    def fourth_phase(n, _):
        @pl.when(n == 2)
        def _():
            wos[0].wait_recv()
            over[0].start()
            came_on[0].start()

        d, z, *f = _tasks([task(n, 3, 3, True), task(n, 3, 2), either(n, 0, 3), either(n, 1, 3)])
        put(OTH, 1, n, _ended(_merge([d, z, _if(late, f[0]), _if(late, f[1])])))
        for j in range(2):
            put(OWN, j, n, _ended(_merge([(ACC[n, j], TOP[n, j]), _if(c == 1, f[j])])))

    def arrive(copies, on):
        for p in range(2):
            copies[p].wait_recv()
            on[p].start()
        for p in range(2):
            on[p].wait_recv()

    for copy in (*got_w, got_t):
        copy.wait()

    def blocks(i, _):
        @pl.when(i == 2)
        def _():
            arrive(first, first_on)

        @pl.when(i == 3)
        def _():
            arrive(second, second_on)

        own = i < 2
        block = jnp.where(own, jnp.where(i == 0, k, 1 - k), i)
        qkv(block, jnp.where(own, 2 * c + block, 2 * (1 - c) + i - 2))
        pair, e = jnp.where(own, OWN, OTH), jnp.where(own, i, jnp.where(i == 2, k, 1 - k))
        for p in range(2):
            X[pair, p, e] = XB(block, half[p], R)[...]

        for at, phase in ((1, second_phase), (2, third_phase), (3, fourth_phase)):

            @pl.when(i == at)
            def _():
                lax.fori_loop(0, HEADS, phase, None)

    lax.fori_loop(0, 4, blocks, None)
    for pair in (OTH, OWN):
        for p in range(2):
            for copy in seen(pair, p):
                copy.start()
    for copy in (hi, lo, *first, *second, *first_on, *second_on):
        copy.wait_send()
    for copy in weights:
        copy.start()

    wos[1].wait_recv()
    over[1].start()
    came_on[1].start()
    for p in range(2):
        over[p].wait_recv()
        lent_on[p].start()
    got_wo.wait()
    for copy in (whole, *came_on, *lent_on):
        copy.wait_recv()
    for copy in weights:
        copy.wait()

    def h_of(pair, p):
        for copy in seen_here(pair, p):
            copy.wait_recv()
        a = S[pair, p].reshape(M, 2048)
        for n in range(0, 2048, TILE):
            at = slice(n, n + TILE)
            h = X[pair, p, :, :, at].reshape(M, TILE).astype(F32) + _dot(a, WO[:, at])
            X[pair, p, :, :, at] = h.astype(BF16).reshape(2, R, TILE)
        hs(pair, p).start()

    def down(out):
        hidden = H[...]
        for n in range(0, 2048, TILE):
            at = slice(n, n + TILE)
            out(n, at, _dot(hidden, WD[:, at]))

    def swapped(ref, p, at):
        return jnp.concatenate([ref[p, R:, at], ref[p, :R, at]], 0).astype(F32)

    def swapped_near(p, at):
        return jnp.concatenate([S[OTH, p, 1, :, at], S[OTH, p, 0, :, at]], 0).astype(F32)

    def step(i, _):
        pair, q, p = lax.div(i, 4), lax.div(i, 2), lax.rem(i, 2)
        e = 1 - lax.rem(q, 2)

        @pl.when(i == 4)
        def _():
            for pair in (OTH, OWN):
                for p in range(2):
                    for copy in seen(pair, p):
                        copy.wait_send()

        @pl.when(lax.rem(i, 4) == 0)
        def _():
            lax.fori_loop(0, 2, lambda p, _: h_of(pair, p), None)

        @pl.when(e == 1)
        def _():
            hs(pair, p).wait_recv()

        B[:R, :] = _normed(X[pair, p, e], gain_m[...][None])
        B[R:, :] = _normed(HS[pair, p, 1 - e], gain_m[...][None])
        b = B[...]
        for n in range(0, 2048, TILE):
            at = slice(n, n + TILE)
            gate, up = _dot(b, WG[:, at]), _dot(b, WU[:, at])
            H[:, at] = (gate * jax.nn.sigmoid(gate) * up).astype(BF16)

        @pl.when(e == 1)
        def _():
            @pl.when(q == 2)
            def _():
                away(p).wait_send()

            def out(n, at, term):
                SA[p, :, at] = term.astype(BF16)

            down(out)

            @pl.when(q == 0)
            def _():
                away(p).start()

            @pl.when(q == 2)
            def _():
                for copy in near(p):
                    copy.start()

        @pl.when(q == 1)
        def _():
            away(p).wait_recv()

            def out(n, at, term):
                SF[p, :, at] = (term + swapped(AW, p, at)).astype(BF16)

            down(out)
            far(p).start()

        @pl.when(q == 3)
        def _():
            for copy in near(p):
                copy.wait_recv()

            def out(n, at, term):
                h = jnp.concatenate([X[OWN, p, 0, :, at], HS[OWN, p, 1, :, at]], 0).astype(F32)
                z = h + term + swapped_near(p, at)
                for j in range(2):
                    ACC[n // 512, j, :HEAD, n % 512 : n % 512 + TILE] = z[j * R : (j + 1) * R]

            down(out)
            far(p).wait_recv()
            for n in range(0, 2048, 512):
                for j in range(2):
                    at = (p, slice(j * R, (j + 1) * R), slice(n, n + 512))
                    AW[at] = (ACC[n // 512, j, :HEAD, :] + FAR[at].astype(F32)).astype(BF16)
            for e in range(2):
                result(p, e).start()

    lax.fori_loop(0, 8, step, None)
    for copy in (*wos, whole, *over, *came_on, *lent_on):
        copy.wait_send()
    for pair in (OTH, OWN):
        for p in range(2):
            hs(pair, p).wait_send()
    for p in range(2):
        far(p).wait_send()
        for copy in near(p):
            copy.wait_send()
        for e in range(2):
            result(p, e).wait()


def _layer(*ins):
    vmem, hbm = pl.BlockSpec(memory_space=pltpu.VMEM), pl.BlockSpec(memory_space=pl.ANY)
    weight = pltpu.VMEM((2048, 2048), BF16)
    pairs = pltpu.VMEM((2, 2, 2, R, 2048), BF16)
    block = pltpu.VMEM((M, 2048), BF16)
    blocks = pltpu.VMEM((2, M, 2048), BF16)
    piece = pltpu.VMEM((2, 2, R, HEADS * HEAD), BF16)
    return pl.pallas_call(
        _body,
        in_specs=[vmem] * 2 + [hbm] * (len(ins) - 2),
        out_specs=hbm,
        out_shape=jax.ShapeDtypeStruct((512, 2048), BF16),
        scratch_shapes=[*[weight] * 4, *[pairs] * 3, block, block, *[blocks] * 4, piece, piece, pltpu.VMEM((2048, HEAD), F32),
                        pltpu.VMEM((HEADS, 2, HEAD + 8, BLOCK), F32), pltpu.VMEM((HEADS, 2, 1, BLOCK), F32),
                        pltpu.SemaphoreType.DMA((13,)), pltpu.SemaphoreType.DMA((43,)), pltpu.SemaphoreType.DMA((43,))],
        compiler_params=pltpu.CompilerParams(collective_id=1, has_side_effects=True, vmem_limit_bytes=67_043_328),
        cost_estimate=pl.CostEstimate(flops=2 * 2048**3 * 4, transcendentals=2**23, bytes_accessed=2**26),
        name="layer",
    )(*ins)


def solution(mesh):
    def step(x, gain_a, wq, wk, wv, wo, gain_m, w_gate, w_up, w_down):
        return _layer(gain_a, gain_m, x, wq, wk, wv, wo, jnp.asarray(_table()), w_gate, w_up, w_down)

    tokens, columns, rows_of = P(("dp", "tp"), None), P(None, "tp"), P("tp", None)
    return jax.shard_map(
        step,
        mesh=mesh,
        in_specs=(tokens, P(None), columns, columns, columns, rows_of, P(None), columns, columns, rows_of),
        out_specs=tokens,
        check_vma=False,
    )
```

```python
import functools

import jax
import jax.numpy as jnp
import numpy as np
from jax import lax
from jax.experimental import pallas as pl
from jax.experimental.pallas import tpu as pltpu
from jax.sharding import PartitionSpec as P

HEAD = 128
HEADS = 4
BLOCK = 512
THETA = 10000
NEG = -1e30
HIDDEN = 2 * NEG
LOG2E = 1.4426950408889634
F32, BF16 = jnp.float32, jnp.bfloat16


def _dot(a, b, ca=1, cb=0):
    return lax.dot_general(a, b, (((ca,), (cb,)), ((), ())), preferred_element_type=F32)


def _normed(x, gain):
    wide = x.astype(F32)
    scale = lax.rsqrt(jnp.mean(wide * wide, -1, keepdims=True) + 1e-6)
    return (wide * scale * gain.astype(F32)).astype(BF16)


def _table():
    half = HEAD // 2
    rate = np.float32(THETA) ** (-np.arange(half, dtype=np.float32) / np.float32(half))
    angle = np.arange(2048, dtype=np.float32)[:, None] * rate.astype(np.float32)
    return np.concatenate([np.cos(angle), np.sin(angle)], 1).astype(np.float32)


E = HEAD**-0.5 * LOG2E


def _scores(q, k, diagonal):
    s = _dot(k, q, 1, 1)
    if diagonal:
        s = jnp.where(lax.broadcasted_iota(jnp.int32, s.shape, 1) >= lax.broadcasted_iota(jnp.int32, s.shape, 0), s, HIDDEN)
    return s


def _tasks(tasks):
    scores = [_scores(q, k, d) for q, k, _, d in tasks]
    out = []
    for (_, _, v, _), s in zip(tasks, scores):
        top = s.max(axis=0, keepdims=True)
        p = jnp.exp2((s - top) * E).astype(BF16)
        out.append((p, top))
    ones = jnp.ones((8, BLOCK), BF16)
    return [(_dot(jnp.concatenate([v, ones], 0), p), top) for (_, _, v, _), (p, top) in zip(tasks, out)]


def _merge(parts):
    top = functools.reduce(jnp.maximum, [t for _, t in parts])
    return sum(a * jnp.exp2((t - top) * E) for a, t in parts), top


def _if(ok, part):
    return part[0], jnp.where(ok, part[1], NEG)


def _ended(part):
    acc = part[0]
    return (acc[:HEAD] * (1 / acc[HEAD : HEAD + 1])).T.astype(BF16)


HB = 1
R = 128
M = 2 * R
TILE = 256
OTH, OWN = 0, 1


def _body(gain_a, gain_m, x, wq, wk, wv, wo, tab, wg, wu, wd, y0, z1, far1, WO, WG, WU, WD, S, X, HS, B, H, SA, SF, AW, FAR, OS, TS, T, ACC, TOP,
          lsem, ssem, rsem):
    t, g = lax.axis_index("tp"), lax.axis_index("dp")
    c, k = lax.div(t, 2), lax.rem(t, 2)
    sib, cross, diag = t + 1 - 2 * k, lax.rem(t + 2, 4), 3 - t
    late = c == 0

    def rows(at, n):
        return pl.ds(pl.multiple_of(at, min(n, R)), n)

    XB = lambda b, at=0, n=BLOCK: WD.at[rows(BLOCK * b + at, n)]
    WQKV = lambda i: WU.at[:, pl.ds(BLOCK * i, BLOCK)]
    KS = lambda b, n: WG.at[rows(BLOCK * b, BLOCK), rows(HEAD * n, HEAD)]
    QS = lambda b, n: WG.at[rows(BLOCK * b, BLOCK), rows(2 * BLOCK + HEAD * n, HEAD)]
    VS = lambda b, n: WG.at[rows(BLOCK * b + HEAD * n, HEAD), pl.ds(BLOCK, BLOCK)]

    def local(i, src, dst):
        return pltpu.make_async_copy(src, dst, lsem.at[i])

    def remote(i, src, dst, to, axis="tp"):
        return pltpu.make_async_remote_copy(
            src, dst, ssem.at[i], rsem.at[i], device_id={axis: to}, device_id_type=pl.DeviceIdType.MESH)

    barrier = pltpu.get_barrier_semaphore()
    for axis, d in (("tp", sib), ("tp", cross), ("tp", diag), ("dp", 1 - g)):
        pl.semaphore_signal(barrier, inc=1, device_id={axis: d}, device_id_type=pl.DeviceIdType.MESH)

    mine, theirs = 512 * t, 512 * cross
    own_rows = rows(mine, 512)
    cols = own_rows
    got_x = local(0, x, XB(k))
    got_w = [local(1 + i, w, WQKV(i)) for i, w in enumerate((wq, wk, wv))]
    got_t = local(4, tab, T)
    got_wo = local(5, wo, WO.at[own_rows])
    weights = [local(6 + i, w, to) for i, (w, to) in enumerate(((wg, WG), (wu, WU), (wd, WD)))]
    hi = remote(0, x.at[pl.ds(256, 256)], XB(k, 256, 256), sib)
    lo = remote(1, x.at[pl.ds(0, 256)], XB(k, 0, 256), sib)
    half = [256 * k + R * p for p in range(2)]
    first = [remote(2 + p, XB(0, half[p], R), XB(2, half[p], R), cross) for p in range(2)]
    direct = [remote(2 + p, x.at[pl.ds(R * p, R)], XB(2, half[p], R), cross) for p in range(2)]
    second = [remote(4 + p, XB(1, half[p], R), XB(3, half[p], R), cross) for p in range(2)]
    first_on = [remote(9 + p, XB(2, half[p], R), XB(2, half[p], R), sib) for p in range(2)]
    second_on = [remote(11 + p, XB(3, half[p], R), XB(3, half[p], R), sib) for p in range(2)]
    few = R // 2
    part = [256 * g + few * n for n in range(4)]
    wos = [remote(i, wo.at[rows(part[n], few)], WO.at[rows(mine + part[n], few)], cross) for n, i in enumerate((6, 7, 44, 45))]
    whole = remote(8, wo, WO.at[own_rows], sib)
    came = [WO.at[rows(theirs + part[n], few)] for n in range(4)]
    lent = [WO.at[rows(theirs + 256 * (1 - g) + few * n, few)] for n in range(4)]
    over = [remote(i, w, w, 1 - g, "dp") for w, i in zip(came, (13, 14, 46, 47))]
    came_on = [remote(i, w, w, sib) for w, i in zip(came, (15, 16, 48, 49))]
    lent_on = [remote(i, w, w, sib) for w, i in zip(lent, (17, 18, 50, 51))]

    def hand_on(n):
        wos[n].wait_recv()
        over[n].start()
        came_on[n].start()

    def seen(pair, p):
        i = 19 + 6 * pair + 3 * p
        to = S.at[pair, p, :, :, cols]
        return [remote(i, (TS if pair == OTH else OS).at[p], to, sib), remote(i + 1, S.at[1 - pair, p, :, :, cols], to, cross),
                remote(i + 2, (OS if pair == OTH else TS).at[p], to, diag)]

    def seen_here(pair, p):
        i = 19 + 6 * pair + 3 * p
        return [remote(i + n, OS.at[p], S.at[pair, p, :, :, cols], sib) for n in range(3)]

    def hs(pair, p):
        return remote(31 + 2 * pair + p, X.at[pair, p], HS.at[pair, p], sib)

    def away(p):
        return remote(35 + p, SA.at[p], AW.at[p], sib)

    far0 = remote(37, SF.at[0], FAR, cross)
    far_rest = [remote(n, SF.at[1, pl.ds(j * R, R)], far1.at[j], cross) for j, n in enumerate((38, 43))]

    def near(p):
        return [remote(39 + 2 * p + j, SA.at[p, pl.ds(j * R, R)], S.at[OTH, p, j], sib) for j in range(2)]

    ended = [local(9 + j, AW.at[0, pl.ds(R * j, R)], y0.at[j]) for j in range(2)]
    ended_z = [local(11 + 2 * n + j, ACC.at[n, j, pl.ds(0, R)], z1.at[j, :, pl.ds(512 * n, 512)]) for n in range(4) for j in range(2)]

    for copy in (got_x, *got_w, got_t, got_wo):
        copy.start()
    pl.semaphore_wait(barrier, 4)
    hi.start()
    lo.start()

    @pl.when(k == 0)
    def _():
        for copy in direct:
            copy.start()

    hi.wait_recv()

    @pl.when(k == 1)
    def _():
        for copy in first:
            copy.start()

    got_x.wait()
    lo.wait_recv()
    for copy in (*second, *wos, whole):
        copy.start()

    def qkv(block, place):
        a = _normed(XB(block)[...], gain_a[...][None])
        SA[0] = a[:M]
        SA[1] = a[M:]
        tt = T[rows(place * BLOCK, BLOCK), :]
        flip = pltpu.roll(tt, HEAD // 2, 1)
        left = lax.broadcasted_iota(jnp.int32, tt.shape, 1) < HEAD // 2
        cos, sin = jnp.where(left, tt, flip), jnp.where(left, -flip, tt)
        a = SA[...].reshape(BLOCK, 2048)
        for h in range(0, HEADS, 2):
            for i, out in enumerate((QS, KS)):
                z2 = _dot(a, WU[:, BLOCK * i + HEAD * h : BLOCK * i + HEAD * (h + 2)]).astype(BF16).astype(F32)
                for n in range(2):
                    z = z2[:, n * HEAD : (n + 1) * HEAD]
                    out(block, h + n)[...] = (z * cos + pltpu.roll(z, HEAD // 2, 1) * sin).astype(BF16)
            v = _dot(a, WU[:, 2 * BLOCK + HEAD * h : 2 * BLOCK + HEAD * (h + 2)]).astype(BF16)
            for n in range(2):
                VS(block, h + n)[...] = v[:, n * HEAD : (n + 1) * HEAD].T

    def task(n, q, kv, diagonal=False):
        return QS(q, n)[...], KS(kv, n)[...], VS(kv, n)[...], diagonal

    def either(n, j, o):
        return task(n, jnp.where(late, o, j), jnp.where(late, j, o))

    def put(pair, j, n, o):
        lo, hi = o[: BLOCK // 2], o[BLOCK // 2 :]
        e = k if j == 0 else 1 - k
        m, s = jnp.where(k == 0, lo, hi), jnp.where(k == 0, hi, lo)
        for p in range(2):
            S[pair, p, e, :, rows(mine + HEAD * n, HEAD)] = m[p * R : (p + 1) * R]
            (OS if pair == OWN else TS)[p, 1 - e, :, rows(HEAD * n, HEAD)] = s[p * R : (p + 1) * R]

    def second_phase(n, _):
        a, *b = _tasks([task(n, 0, 0, True), task(n, 1, 0), task(n, 1, 1, True)])
        for j, (acc, top) in enumerate((a, _merge(b))):
            ACC[n, j], TOP[n, j] = acc, top

    def third_phase(n, _):
        d, *f = _tasks([task(n, 2, 2, True), either(n, 0, 2), either(n, 1, 2)])
        put(OTH, 0, n, _ended(_merge([d, _if(late, f[0]), _if(late, f[1])])))
        for j in range(2):
            ACC[n, j], TOP[n, j] = _merge([(ACC[n, j], TOP[n, j]), _if(c == 1, f[j])])

    def fourth_phase(n, _):
        for piece in range(2):

            @pl.when(n == 2 * piece + 1)
            def _():
                hand_on(piece)

        d, z, *f = _tasks([task(n, 3, 3, True), task(n, 3, 2), either(n, 0, 3), either(n, 1, 3)])
        put(OTH, 1, n, _ended(_merge([d, z, _if(late, f[0]), _if(late, f[1])])))
        for j in range(2):
            put(OWN, j, n, _ended(_merge([(ACC[n, j], TOP[n, j]), _if(c == 1, f[j])])))

    def arrive(copies, on):
        for p in range(2):
            copies[p].wait_recv()
            on[p].start()
        for p in range(2):
            on[p].wait_recv()

    for copy in (*got_w, got_t):
        copy.wait()

    def blocks(i, _):
        @pl.when(i == 2)
        def _():
            arrive(first, first_on)

        @pl.when(i == 3)
        def _():
            arrive(second, second_on)

        own = i < 2
        block = jnp.where(own, jnp.where(i == 0, k, 1 - k), i)
        qkv(block, jnp.where(own, 2 * c + block, 2 * (1 - c) + i - 2))
        pair, e = jnp.where(own, OWN, OTH), jnp.where(own, i, jnp.where(i == 2, k, 1 - k))
        for p in range(2):
            X[pair, p, e] = XB(block, half[p], R)[...]

        for at, phase in ((1, second_phase), (2, third_phase), (3, fourth_phase)):

            @pl.when(i == at)
            def _():
                lax.fori_loop(0, HEADS, phase, None)

    lax.fori_loop(0, 4, blocks, None)
    for copy in seen(OTH, 0):
        copy.start()
    hand_on(2)
    for copy in (hi, lo, *first, *second, *first_on, *second_on):
        copy.wait_send()
    for copy in weights:
        copy.start()

    hand_on(3)
    for copy in seen(OTH, 1):
        copy.start()
    for n in range(4):
        over[n].wait_recv()
        lent_on[n].start()
    for p in range(2):
        for copy in seen(OWN, p):
            copy.start()
    got_wo.wait()
    for copy in (whole, *came_on, *lent_on):
        copy.wait_recv()
    for copy in weights:
        copy.wait()

    def h_of(pair, p):
        for copy in seen_here(pair, p):
            copy.wait_recv()
        a = S[pair, p].reshape(M, 2048)
        for n in range(0, 2048, TILE):
            at = slice(n, n + TILE)
            h = X[pair, p, :, :, at].reshape(M, TILE).astype(F32) + _dot(a, WO[:, at])
            X[pair, p, :, :, at] = h.astype(BF16).reshape(2, R, TILE)
        hs(pair, p).start()

    def down(out):
        hidden = H[...]
        for n in range(0, 2048, TILE):
            at = slice(n, n + TILE)
            out(n, at, _dot(hidden, WD[:, at]))

    def swapped(ref, p, at):
        return jnp.concatenate([ref[p, R:, at], ref[p, :R, at]], 0).astype(F32)

    def swapped_near(p, at):
        return jnp.concatenate([S[OTH, p, 1, :, at], S[OTH, p, 0, :, at]], 0).astype(F32)

    def step(i, _):
        pair, q, p = lax.div(i, 4), lax.div(i, 2), lax.rem(i, 2)
        e = 1 - lax.rem(q, 2)

        @pl.when(e == 1)
        def _():
            hs(pair, p).wait_recv()

        B[:R, :] = _normed(X[pair, p, e], gain_m[...][None])
        B[R:, :] = _normed(HS[pair, p, 1 - e], gain_m[...][None])
        b = B[...]
        for n in range(0, 2048, TILE):
            at = slice(n, n + TILE)
            gate, up = _dot(b, WG[:, at]), _dot(b, WU[:, at])
            H[:, at] = (gate * jax.nn.sigmoid(gate) * up).astype(BF16)

        for p_, at in ((0, 3), (1, 4)):

            @pl.when(i == at)
            def _():
                for copy in (*seen(OTH, p_), *seen(OWN, p_)):
                    copy.wait_send()

        @pl.when((i == 0) | (i == 3) | (i == 4))
        def _():
            h_of(jnp.where(i == 0, OTH, OWN), jnp.where(i == 3, 0, 1))

        @pl.when(e == 1)
        def _():
            @pl.when(q == 2)
            def _():
                away(p).wait_send()

            def out(n, at, term):
                SA[p, :, at] = term.astype(BF16)

            down(out)

            @pl.when(q == 0)
            def _():
                away(p).start()

            @pl.when(q == 2)
            def _():
                for copy in near(p):
                    copy.start()

        @pl.when(q == 1)
        def _():
            away(p).wait_recv()

            def out(n, at, term):
                SF[p, :, at] = (term + swapped(AW, p, at)).astype(BF16)

            down(out)

            @pl.when(p == 0)
            def _():
                far0.start()

            @pl.when(p == 1)
            def _():
                for copy in far_rest:
                    copy.start()

        @pl.when(q == 3)
        def _():
            for copy in near(p):
                copy.wait_recv()

            def out(n, at, term):
                h = jnp.concatenate([X[OWN, p, 0, :, at], HS[OWN, p, 1, :, at]], 0).astype(F32)
                z = h + term + swapped_near(p, at)
                for j in range(2):
                    ACC[n // 512, j, :HEAD, n % 512 : n % 512 + TILE] = z[j * R : (j + 1) * R]

            down(out)

            @pl.when(p == 0)
            def _():
                far0.wait_recv()
                for n in range(0, 2048, 512):
                    for j in range(2):
                        r, at = slice(j * R, (j + 1) * R), slice(n, n + 512)
                        AW[0, r, at] = (ACC[n // 512, j, :HEAD, :] + FAR[r, at].astype(F32)).astype(BF16)
                for copy in ended:
                    copy.start()
                for copy in ended:
                    copy.wait()

            @pl.when(p == 1)
            def _():
                for copy in ended_z:
                    copy.start()

    h_of(OTH, 0)
    lax.fori_loop(0, 8, step, None)
    for copy in (*wos, whole, *over, *came_on, *lent_on):
        copy.wait_send()
    for pair in (OTH, OWN):
        for p in range(2):
            hs(pair, p).wait_send()
    far0.wait_send()
    for copy in far_rest:
        copy.wait()
    for p in range(2):
        for copy in near(p):
            copy.wait_send()
    for copy in ended_z:
        copy.wait()


def _layer(*ins):
    vmem, hbm = pl.BlockSpec(memory_space=pltpu.VMEM), pl.BlockSpec(memory_space=pl.ANY)
    weight = pltpu.VMEM((2048, 2048), BF16)
    pairs = pltpu.VMEM((2, 2, 2, R, 2048), BF16)
    block = pltpu.VMEM((M, 2048), BF16)
    blocks = pltpu.VMEM((2, M, 2048), BF16)
    piece = pltpu.VMEM((2, 2, R, HEADS * HEAD), BF16)
    return pl.pallas_call(
        _body,
        in_specs=[vmem] * 2 + [hbm] * (len(ins) - 2),
        out_specs=[hbm] * 3,
        out_shape=[jax.ShapeDtypeStruct((2, R, 2048), d) for d in (BF16, F32, BF16)],
        scratch_shapes=[*[weight] * 4, *[pairs] * 3, block, block, *[blocks] * 3, block, piece, piece, pltpu.VMEM((2048, HEAD), F32),
                        pltpu.VMEM((HEADS, 2, HEAD + 8, BLOCK), F32), pltpu.VMEM((HEADS, 2, 1, BLOCK), F32),
                        pltpu.SemaphoreType.DMA((19,)), pltpu.SemaphoreType.DMA((52,)), pltpu.SemaphoreType.DMA((52,))],
        compiler_params=pltpu.CompilerParams(collective_id=1, has_side_effects=True, vmem_limit_bytes=67_043_328),
        cost_estimate=pl.CostEstimate(flops=2 * 2048**3 * 4, transcendentals=2**23, bytes_accessed=2**26),
        name="layer",
    )(*ins)


def _end_body(y0, z1, far1, y, A, Z, F, rsem, wsem):
    k = lax.rem(lax.axis_index("tp"), 2)
    loads = [pltpu.make_async_copy(a, b, rsem.at[3 * j + i])
             for j in range(2) for i, (a, b) in enumerate(((z1.at[j], Z.at[j]), (far1.at[j], F.at[j]), (y0.at[j], A.at[0, j])))]
    stores = [pltpu.make_async_copy(A.at[p, j], y.at[pl.ds(pl.multiple_of(256 * (k if j == 0 else 1 - k) + R * p, R), R)], wsem.at[2 * p + j])
              for p in range(2) for j in range(2)]
    for copy in loads:
        copy.start()
    for j in range(2):
        loads[3 * j].wait()
        loads[3 * j + 1].wait()
        A[1, j] = (Z[j] + F[j].astype(F32)).astype(BF16)
        stores[2 + j].start()
        loads[3 * j + 2].wait()
        stores[j].start()
    for copy in stores:
        copy.wait()


def _end(*ins):
    hbm = pl.BlockSpec(memory_space=pl.ANY)
    return pl.pallas_call(
        _end_body,
        in_specs=[hbm] * 3,
        out_specs=hbm,
        out_shape=jax.ShapeDtypeStruct((512, 2048), BF16),
        scratch_shapes=[pltpu.VMEM((2, 2, R, 2048), BF16), pltpu.VMEM((2, R, 2048), F32), pltpu.VMEM((2, R, 2048), BF16),
                        pltpu.SemaphoreType.DMA((6,)), pltpu.SemaphoreType.DMA((4,))],
        compiler_params=pltpu.CompilerParams(vmem_limit_bytes=67_043_328),
        cost_estimate=pl.CostEstimate(flops=2**20, transcendentals=0, bytes_accessed=6 * 2**20),
        name="end",
    )(*ins)


def solution(mesh):
    def step(x, gain_a, wq, wk, wv, wo, gain_m, w_gate, w_up, w_down):
        return _end(*_layer(gain_a, gain_m, x, wq, wk, wv, wo, jnp.asarray(_table()), w_gate, w_up, w_down))

    tokens, columns, rows_of = P(("dp", "tp"), None), P(None, "tp"), P("tp", None)
    return jax.shard_map(
        step,
        mesh=mesh,
        in_specs=(tokens, P(None), columns, columns, columns, rows_of, P(None), columns, columns, rows_of),
        out_specs=tokens,
        check_vma=False,
    )
```

```python
import functools

import jax
import jax.numpy as jnp
import numpy as np
from jax import lax
from jax.experimental import pallas as pl
from jax.experimental.pallas import tpu as pltpu
from jax.sharding import PartitionSpec as P

HEAD = 128
HEADS = 4
BLOCK = 512
THETA = 10000
NEG = -1e30
HIDDEN = 2 * NEG
LOG2E = 1.4426950408889634
F32, BF16 = jnp.float32, jnp.bfloat16


def _dot(a, b, ca=1, cb=0):
    return lax.dot_general(a, b, (((ca,), (cb,)), ((), ())), preferred_element_type=F32)


def _normed(x, gain):
    wide = x.astype(F32)
    scale = lax.rsqrt(jnp.mean(wide * wide, -1, keepdims=True) + 1e-6)
    return (wide * scale * gain.astype(F32)).astype(BF16)


def _table():
    half = HEAD // 2
    rate = np.float32(THETA) ** (-np.arange(half, dtype=np.float32) / np.float32(half))
    angle = np.arange(2048, dtype=np.float32)[:, None] * rate.astype(np.float32)
    return np.concatenate([np.cos(angle), np.sin(angle)], 1).astype(np.float32)


E = HEAD**-0.5 * LOG2E


def _scores(q, k, diagonal):
    s = _dot(k, q, 1, 1)
    if diagonal:
        s = jnp.where(lax.broadcasted_iota(jnp.int32, s.shape, 1) >= lax.broadcasted_iota(jnp.int32, s.shape, 0), s, HIDDEN)
    return s


def _tasks(tasks):
    scores = [_scores(q, k, d) for q, k, _, d in tasks]
    out = []
    for (_, _, v, _), s in zip(tasks, scores):
        top = s.max(axis=0, keepdims=True)
        p = jnp.exp2((s - top) * E).astype(BF16)
        out.append((p, top))
    ones = jnp.ones((8, BLOCK), BF16)
    return [(_dot(jnp.concatenate([v, ones], 0), p), top) for (_, _, v, _), (p, top) in zip(tasks, out)]


def _merge(parts):
    top = functools.reduce(jnp.maximum, [t for _, t in parts])
    return sum(a * jnp.exp2((t - top) * E) for a, t in parts), top


def _if(ok, part):
    return part[0], jnp.where(ok, part[1], NEG)


def _ended(part):
    acc = part[0]
    return (acc[:HEAD] * (1 / acc[HEAD : HEAD + 1])).T.astype(BF16)


HB = 1
R = 128
M = 2 * R
TILE = 256
OTH, OWN = 0, 1


def _body(gain_a, gain_m, x, wq, wk, wv, wo, tab, wg, wu, wd, y0, z1, far1, WO, WG, WU, WD, S, X, HS, B, H, SA, SF, AW, FAR, OS, TS, T, ACC, TOP,
          lsem, ssem, rsem):
    t, g = lax.axis_index("tp"), lax.axis_index("dp")
    c, k = lax.div(t, 2), lax.rem(t, 2)
    sib, cross, diag = t + 1 - 2 * k, lax.rem(t + 2, 4), 3 - t
    late = c == 0

    def rows(at, n):
        return pl.ds(pl.multiple_of(at, min(n, R)), n)

    XB = lambda b, at=0, n=BLOCK: WD.at[rows(BLOCK * b + at, n)]
    WQKV = lambda i: WU.at[:, pl.ds(BLOCK * i, BLOCK)]
    KS = lambda b, n: WG.at[rows(BLOCK * b, BLOCK), rows(HEAD * n, HEAD)]
    QS = lambda b, n: WG.at[rows(BLOCK * b, BLOCK), rows(2 * BLOCK + HEAD * n, HEAD)]
    VS = lambda b, n: WG.at[rows(BLOCK * b + HEAD * n, HEAD), pl.ds(BLOCK, BLOCK)]

    def local(i, src, dst):
        return pltpu.make_async_copy(src, dst, lsem.at[i])

    def remote(i, src, dst, to, axis="tp"):
        return pltpu.make_async_remote_copy(
            src, dst, ssem.at[i], rsem.at[i], device_id={axis: to}, device_id_type=pl.DeviceIdType.MESH)

    barrier = pltpu.get_barrier_semaphore()
    for axis, d in (("tp", sib), ("tp", cross), ("tp", diag), ("dp", 1 - g)):
        pl.semaphore_signal(barrier, inc=1, device_id={axis: d}, device_id_type=pl.DeviceIdType.MESH)

    mine, theirs = 512 * t, 512 * cross
    own_rows = rows(mine, 512)
    cols = own_rows
    got_x = local(0, x, XB(k))
    got_w = [local(1 + i, w, WQKV(i)) for i, w in enumerate((wq, wk, wv))]
    got_t = local(4, tab, T)
    got_wo = local(5, wo, WO.at[own_rows])
    weights = [local(6 + i, w, to) for i, (w, to) in enumerate(((wg, WG), (wu, WU), (wd, WD)))]
    hi = remote(0, x.at[pl.ds(256, 256)], XB(k, 256, 256), sib)
    lo = remote(1, x.at[pl.ds(0, 256)], XB(k, 0, 256), sib)
    half = [256 * k + R * p for p in range(2)]
    first = [remote(2 + p, XB(0, half[p], R), XB(2, half[p], R), cross) for p in range(2)]
    direct = [remote(2 + p, x.at[pl.ds(R * p, R)], XB(2, half[p], R), cross) for p in range(2)]
    second = [remote(4 + p, XB(1, half[p], R), XB(3, half[p], R), cross) for p in range(2)]
    first_on = [remote(9 + p, XB(2, half[p], R), XB(2, half[p], R), sib) for p in range(2)]
    second_on = [remote(11 + p, XB(3, half[p], R), XB(3, half[p], R), sib) for p in range(2)]
    few = R // 2
    part = [256 * g + few * n for n in range(4)]
    wos = [remote(i, wo.at[rows(part[n], few)], WO.at[rows(mine + part[n], few)], cross) for n, i in enumerate((6, 7, 44, 45))]
    whole = remote(8, wo, WO.at[own_rows], sib)
    came = [WO.at[rows(theirs + part[n], few)] for n in range(4)]
    lent = [WO.at[rows(theirs + 256 * (1 - g) + few * n, few)] for n in range(4)]
    over = [remote(i, w, w, 1 - g, "dp") for w, i in zip(came, (13, 14, 46, 47))]
    came_on = [remote(i, w, w, sib) for w, i in zip(came, (15, 16, 48, 49))]
    lent_on = [remote(i, w, w, sib) for w, i in zip(lent, (17, 18, 50, 51))]

    def hand_on(n):
        wos[n].wait_recv()
        over[n].start()
        came_on[n].start()

    def seen(pair, p):
        i = 19 + 6 * pair + 3 * p
        to = S.at[pair, p, :, :, cols]
        return [remote(i, (TS if pair == OTH else OS).at[p], to, sib), remote(i + 1, S.at[1 - pair, p, :, :, cols], to, cross),
                remote(i + 2, (OS if pair == OTH else TS).at[p], to, diag)]

    def seen_here(pair, p):
        i = 19 + 6 * pair + 3 * p
        return [remote(i + n, OS.at[p], S.at[pair, p, :, :, cols], sib) for n in range(3)]

    def hs(pair, p):
        return remote(31 + 2 * pair + p, X.at[pair, p], HS.at[pair, p], sib)

    def away(p):
        return remote(35 + p, SA.at[p], AW.at[p], sib)

    far0 = remote(37, SF.at[0], FAR, cross)
    far_rest = [remote(n, SF.at[1, pl.ds(j * R, R)], far1.at[j], cross) for j, n in enumerate((38, 43))]

    def near(p):
        return [remote(39 + 2 * p + j, SA.at[p, pl.ds(j * R, R)], S.at[OTH, p, j], sib) for j in range(2)]

    ended = [local(9 + j, AW.at[0, pl.ds(R * j, R)], y0.at[j]) for j in range(2)]
    ended_z = [local(11 + 2 * n + j, ACC.at[n, j, pl.ds(0, R)], z1.at[j, :, pl.ds(512 * n, 512)]) for n in range(4) for j in range(2)]

    for copy in (got_x, *got_w, got_t, got_wo):
        copy.start()
    pl.semaphore_wait(barrier, 4)
    hi.start()
    lo.start()

    @pl.when(k == 0)
    def _():
        for copy in direct:
            copy.start()

    hi.wait_recv()

    @pl.when(k == 1)
    def _():
        for copy in first:
            copy.start()

    got_x.wait()
    lo.wait_recv()
    for copy in (*second, *wos, whole):
        copy.start()

    def qkv(block, place):
        a = _normed(XB(block)[...], gain_a[...][None])
        SA[0] = a[:M]
        SA[1] = a[M:]
        tt = T[rows(place * BLOCK, BLOCK), :]
        flip = pltpu.roll(tt, HEAD // 2, 1)
        left = lax.broadcasted_iota(jnp.int32, tt.shape, 1) < HEAD // 2
        cos, sin = jnp.where(left, tt, flip), jnp.where(left, -flip, tt)
        a = SA[...].reshape(BLOCK, 2048)
        for h in range(0, HEADS, 2):
            for i, out in enumerate((QS, KS)):
                z2 = _dot(a, WU[:, BLOCK * i + HEAD * h : BLOCK * i + HEAD * (h + 2)]).astype(BF16).astype(F32)
                for n in range(2):
                    z = z2[:, n * HEAD : (n + 1) * HEAD]
                    out(block, h + n)[...] = (z * cos + pltpu.roll(z, HEAD // 2, 1) * sin).astype(BF16)
            v = _dot(a, WU[:, 2 * BLOCK + HEAD * h : 2 * BLOCK + HEAD * (h + 2)]).astype(BF16)
            for n in range(2):
                VS(block, h + n)[...] = v[:, n * HEAD : (n + 1) * HEAD].T

    def task(n, q, kv, diagonal=False):
        return QS(q, n)[...], KS(kv, n)[...], VS(kv, n)[...], diagonal

    def either(n, j, o):
        return task(n, jnp.where(late, o, j), jnp.where(late, j, o))

    def put(pair, j, n, o):
        lo, hi = o[: BLOCK // 2], o[BLOCK // 2 :]
        e = k if j == 0 else 1 - k
        m, s = jnp.where(k == 0, lo, hi), jnp.where(k == 0, hi, lo)
        for p in range(2):
            S[pair, p, e, :, rows(mine + HEAD * n, HEAD)] = m[p * R : (p + 1) * R]
            (OS if pair == OWN else TS)[p, 1 - e, :, rows(HEAD * n, HEAD)] = s[p * R : (p + 1) * R]

    def second_phase(n, _):
        a, *b = _tasks([task(n, 0, 0, True), task(n, 1, 0), task(n, 1, 1, True)])
        for j, (acc, top) in enumerate((a, _merge(b))):
            ACC[n, j], TOP[n, j] = acc, top

    def third_phase(n, _):
        d, *f = _tasks([task(n, 2, 2, True), either(n, 0, 2), either(n, 1, 2)])
        put(OTH, 0, n, _ended(_merge([d, _if(late, f[0]), _if(late, f[1])])))
        for j in range(2):
            ACC[n, j], TOP[n, j] = _merge([(ACC[n, j], TOP[n, j]), _if(c == 1, f[j])])

    def fourth_phase(n, _):
        for piece in range(2):

            @pl.when(n == 2 * piece + 1)
            def _():
                hand_on(piece)

        d, z, *f = _tasks([task(n, 3, 3, True), task(n, 3, 2), either(n, 0, 3), either(n, 1, 3)])
        put(OTH, 1, n, _ended(_merge([d, z, _if(late, f[0]), _if(late, f[1])])))
        for j in range(2):
            put(OWN, j, n, _ended(_merge([(ACC[n, j], TOP[n, j]), _if(c == 1, f[j])])))

    def arrive(copies, on):
        for p in range(2):
            copies[p].wait_recv()
            on[p].start()
        for p in range(2):
            on[p].wait_recv()

    for copy in (*got_w, got_t):
        copy.wait()

    def blocks(i, _):
        @pl.when(i == 2)
        def _():
            arrive(first, first_on)

        @pl.when(i == 3)
        def _():
            arrive(second, second_on)

        own = i < 2
        block = jnp.where(own, jnp.where(i == 0, k, 1 - k), i)
        qkv(block, jnp.where(own, 2 * c + block, 2 * (1 - c) + i - 2))
        pair, e = jnp.where(own, OWN, OTH), jnp.where(own, i, jnp.where(i == 2, k, 1 - k))
        for p in range(2):
            X[pair, p, e] = XB(block, half[p], R)[...]

        for at, phase in ((1, second_phase), (2, third_phase), (3, fourth_phase)):

            @pl.when(i == at)
            def _():
                lax.fori_loop(0, HEADS, phase, None)

    lax.fori_loop(0, 4, blocks, None)
    for copy in seen(OTH, 0):
        copy.start()
    hand_on(2)
    for copy in (hi, lo, *first, *second, *first_on, *second_on):
        copy.wait_send()
    for copy in weights:
        copy.start()

    hand_on(3)
    for copy in seen(OTH, 1):
        copy.start()
    for n in range(4):
        over[n].wait_recv()
        lent_on[n].start()
    for p in range(2):
        for copy in seen(OWN, p):
            copy.start()
    got_wo.wait()
    for copy in (whole, *came_on, *lent_on):
        copy.wait_recv()
    for copy in weights:
        copy.wait()

    def h_of(pair, p):
        for copy in seen_here(pair, p):
            copy.wait_recv()
        a = S[pair, p].reshape(M, 2048)
        for n in range(0, 2048, TILE):
            at = slice(n, n + TILE)
            h = X[pair, p, :, :, at].reshape(M, TILE).astype(F32) + _dot(a, WO[:, at])
            X[pair, p, :, :, at] = h.astype(BF16).reshape(2, R, TILE)
        hs(pair, p).start()

    def down(out):
        hidden = H[...]
        for n in range(0, 2048, TILE):
            at = slice(n, n + TILE)
            out(n, at, _dot(hidden, WD[:, at]))

    def swapped(ref, p, at):
        return jnp.concatenate([ref[p, R:, at], ref[p, :R, at]], 0).astype(F32)

    def swapped_near(p, at):
        return jnp.concatenate([S[OTH, p, 1, :, at], S[OTH, p, 0, :, at]], 0).astype(F32)

    def step(i, _):
        pair, p, e = lax.div(i, 4), lax.rem(lax.div(i, 2), 2), 1 - lax.rem(i, 2)
        q = 2 * pair + 1 - e

        @pl.when(e == 1)
        def _():
            hs(pair, p).wait_recv()

        B[:R, :] = _normed(X[pair, p, e], gain_m[...][None])
        B[R:, :] = _normed(HS[pair, p, 1 - e], gain_m[...][None])
        b = B[...]
        for n in range(0, 2048, TILE):
            at = slice(n, n + TILE)
            gate, up = _dot(b, WG[:, at]), _dot(b, WU[:, at])
            H[:, at] = (gate * jax.nn.sigmoid(gate) * up).astype(BF16)

        for p_, at in ((0, 3), (1, 5)):

            @pl.when(i == at)
            def _():
                for copy in (*seen(OTH, p_), *seen(OWN, p_)):
                    copy.wait_send()

        @pl.when((i == 1) | (i == 3) | (i == 5))
        def _():
            h_of(jnp.where(i == 1, OTH, OWN), jnp.where(i == 3, 0, 1))

        @pl.when(e == 1)
        def _():
            @pl.when(q == 2)
            def _():
                away(p).wait_send()

            def out(n, at, term):
                SA[p, :, at] = term.astype(BF16)

            down(out)

            @pl.when(q == 0)
            def _():
                away(p).start()

            @pl.when(q == 2)
            def _():
                for copy in near(p):
                    copy.start()

        @pl.when(q == 1)
        def _():
            away(p).wait_recv()

            def out(n, at, term):
                SF[p, :, at] = (term + swapped(AW, p, at)).astype(BF16)

            down(out)

            @pl.when(p == 0)
            def _():
                far0.start()

            @pl.when(p == 1)
            def _():
                for copy in far_rest:
                    copy.start()

        @pl.when(q == 3)
        def _():
            for copy in near(p):
                copy.wait_recv()

            def out(n, at, term):
                h = jnp.concatenate([X[OWN, p, 0, :, at], HS[OWN, p, 1, :, at]], 0).astype(F32)
                z = h + term + swapped_near(p, at)
                for j in range(2):
                    ACC[n // 512, j, :HEAD, n % 512 : n % 512 + TILE] = z[j * R : (j + 1) * R]

            down(out)

            @pl.when(p == 0)
            def _():
                far0.wait_recv()
                for n in range(0, 2048, 512):
                    for j in range(2):
                        r, at = slice(j * R, (j + 1) * R), slice(n, n + 512)
                        AW[0, r, at] = (ACC[n // 512, j, :HEAD, :] + FAR[r, at].astype(F32)).astype(BF16)
                for copy in ended:
                    copy.start()
                for copy in ended:
                    copy.wait()

            @pl.when(p == 1)
            def _():
                for copy in ended_z:
                    copy.start()

    h_of(OTH, 0)
    lax.fori_loop(0, 8, step, None)
    for copy in (*wos, whole, *over, *came_on, *lent_on):
        copy.wait_send()
    for pair in (OTH, OWN):
        for p in range(2):
            hs(pair, p).wait_send()
    far0.wait_send()
    for copy in far_rest:
        copy.wait()
    for p in range(2):
        for copy in near(p):
            copy.wait_send()
    for copy in ended_z:
        copy.wait()


def _layer(*ins):
    vmem, hbm = pl.BlockSpec(memory_space=pltpu.VMEM), pl.BlockSpec(memory_space=pl.ANY)
    weight = pltpu.VMEM((2048, 2048), BF16)
    pairs = pltpu.VMEM((2, 2, 2, R, 2048), BF16)
    block = pltpu.VMEM((M, 2048), BF16)
    blocks = pltpu.VMEM((2, M, 2048), BF16)
    piece = pltpu.VMEM((2, 2, R, HEADS * HEAD), BF16)
    return pl.pallas_call(
        _body,
        in_specs=[vmem] * 2 + [hbm] * (len(ins) - 2),
        out_specs=[hbm] * 3,
        out_shape=[jax.ShapeDtypeStruct((2, R, 2048), d) for d in (BF16, F32, BF16)],
        scratch_shapes=[*[weight] * 4, *[pairs] * 3, block, block, *[blocks] * 3, block, piece, piece, pltpu.VMEM((2048, HEAD), F32),
                        pltpu.VMEM((HEADS, 2, HEAD + 8, BLOCK), F32), pltpu.VMEM((HEADS, 2, 1, BLOCK), F32),
                        pltpu.SemaphoreType.DMA((19,)), pltpu.SemaphoreType.DMA((52,)), pltpu.SemaphoreType.DMA((52,))],
        compiler_params=pltpu.CompilerParams(collective_id=1, has_side_effects=True, vmem_limit_bytes=67_043_328),
        cost_estimate=pl.CostEstimate(flops=2 * 2048**3 * 4, transcendentals=2**23, bytes_accessed=2**26),
        name="layer",
    )(*ins)


def _end_body(y0, z1, far1, y, A, Z, F, rsem, wsem):
    k = lax.rem(lax.axis_index("tp"), 2)
    loads = [pltpu.make_async_copy(a, b, rsem.at[3 * j + i])
             for j in range(2) for i, (a, b) in enumerate(((z1.at[j], Z.at[j]), (far1.at[j], F.at[j]), (y0.at[j], A.at[0, j])))]
    stores = [pltpu.make_async_copy(A.at[p, j], y.at[pl.ds(pl.multiple_of(256 * (k if j == 0 else 1 - k) + R * p, R), R)], wsem.at[2 * p + j])
              for p in range(2) for j in range(2)]
    for copy in loads:
        copy.start()
    for j in range(2):
        loads[3 * j].wait()
        loads[3 * j + 1].wait()
        A[1, j] = (Z[j] + F[j].astype(F32)).astype(BF16)
        stores[2 + j].start()
        loads[3 * j + 2].wait()
        stores[j].start()
    for copy in stores:
        copy.wait()


def _end(*ins):
    hbm = pl.BlockSpec(memory_space=pl.ANY)
    return pl.pallas_call(
        _end_body,
        in_specs=[hbm] * 3,
        out_specs=hbm,
        out_shape=jax.ShapeDtypeStruct((512, 2048), BF16),
        scratch_shapes=[pltpu.VMEM((2, 2, R, 2048), BF16), pltpu.VMEM((2, R, 2048), F32), pltpu.VMEM((2, R, 2048), BF16),
                        pltpu.SemaphoreType.DMA((6,)), pltpu.SemaphoreType.DMA((4,))],
        compiler_params=pltpu.CompilerParams(vmem_limit_bytes=67_043_328),
        cost_estimate=pl.CostEstimate(flops=2**20, transcendentals=0, bytes_accessed=6 * 2**20),
        name="end",
    )(*ins)


def solution(mesh):
    def step(x, gain_a, wq, wk, wv, wo, gain_m, w_gate, w_up, w_down):
        return _end(*_layer(gain_a, gain_m, x, wq, wk, wv, wo, jnp.asarray(_table()), w_gate, w_up, w_down))

    tokens, columns, rows_of = P(("dp", "tp"), None), P(None, "tp"), P("tp", None)
    return jax.shard_map(
        step,
        mesh=mesh,
        in_specs=(tokens, P(None), columns, columns, columns, rows_of, P(None), columns, columns, rows_of),
        out_specs=tokens,
        check_vma=False,
    )
```

```python
import functools

import jax
import jax.numpy as jnp
import numpy as np
from jax import lax
from jax.experimental import pallas as pl
from jax.experimental.pallas import tpu as pltpu
from jax.sharding import PartitionSpec as P

HEAD = 128
HEADS = 4
BLOCK = 512
THETA = 10000
NEG = -1e30
HIDDEN = 2 * NEG
LOG2E = 1.4426950408889634
F32, BF16 = jnp.float32, jnp.bfloat16


def _dot(a, b, ca=1, cb=0):
    return lax.dot_general(a, b, (((ca,), (cb,)), ((), ())), preferred_element_type=F32)


def _normed(x, gain):
    wide = x.astype(F32)
    scale = lax.rsqrt(jnp.mean(wide * wide, -1, keepdims=True) + 1e-6)
    return (wide * scale * gain.astype(F32)).astype(BF16)


def _table():
    half = HEAD // 2
    rate = np.float32(THETA) ** (-np.arange(half, dtype=np.float32) / np.float32(half))
    angle = np.arange(2048, dtype=np.float32)[:, None] * rate.astype(np.float32)
    return np.concatenate([np.cos(angle), np.sin(angle)], 1).astype(np.float32)


E = HEAD**-0.5 * LOG2E


def _scores(q, k, diagonal):
    s = _dot(k, q, 1, 1)
    if diagonal:
        s = jnp.where(lax.broadcasted_iota(jnp.int32, s.shape, 1) >= lax.broadcasted_iota(jnp.int32, s.shape, 0), s, HIDDEN)
    return s


def _tasks(tasks):
    scores = [_scores(q, k, d) for q, k, _, d in tasks]
    out = []
    for (_, _, v, _), s in zip(tasks, scores):
        top = s.max(axis=0, keepdims=True)
        p = jnp.exp2((s - top) * E).astype(BF16)
        out.append((p, top))
    ones = jnp.ones((8, BLOCK), BF16)
    return [(_dot(jnp.concatenate([v, ones], 0), p), top) for (_, _, v, _), (p, top) in zip(tasks, out)]


def _merge(parts):
    top = functools.reduce(jnp.maximum, [t for _, t in parts])
    return sum(a * jnp.exp2((t - top) * E) for a, t in parts), top


def _if(ok, part):
    return part[0], jnp.where(ok, part[1], NEG)


def _ended(part):
    acc = part[0]
    return (acc[:HEAD] * (1 / acc[HEAD : HEAD + 1])).T.astype(BF16)


HB = 1
R = 128
M = 2 * R
TILE = 256
OTH, OWN = 0, 1


def _body(gain_a_in, gain_m_in, x, wq, wk, wv, wo, tab, wg, wu, wd, y0, z1, far1, WO, WG, WU, WD, S, X, HS, B, H, SA, SF, AW, FAR, OS, TS, T, ACC, TOP,
          gain_a, gain_m, lsem, ssem, rsem):
    t, g = lax.axis_index("tp"), lax.axis_index("dp")
    c, k = lax.div(t, 2), lax.rem(t, 2)
    sib, cross, diag = t + 1 - 2 * k, lax.rem(t + 2, 4), 3 - t
    late = c == 0

    def rows(at, n):
        return pl.ds(pl.multiple_of(at, min(n, R)), n)

    XB = lambda b, at=0, n=BLOCK: WD.at[rows(BLOCK * b + at, n)]
    WQKV = lambda i: WU.at[:, pl.ds(BLOCK * i, BLOCK)]
    KS = lambda b, n: WG.at[rows(BLOCK * b, BLOCK), rows(HEAD * n, HEAD)]
    QS = lambda b, n: WG.at[rows(BLOCK * b, BLOCK), rows(2 * BLOCK + HEAD * n, HEAD)]
    VS = lambda b, n: WG.at[rows(BLOCK * b + HEAD * n, HEAD), pl.ds(BLOCK, BLOCK)]

    def local(i, src, dst):
        return pltpu.make_async_copy(src, dst, lsem.at[i])

    def remote(i, src, dst, to, axis="tp"):
        return pltpu.make_async_remote_copy(
            src, dst, ssem.at[i], rsem.at[i], device_id={axis: to}, device_id_type=pl.DeviceIdType.MESH)

    barrier = pltpu.get_barrier_semaphore()
    for axis, d in (("tp", sib), ("tp", cross), ("tp", diag), ("dp", 1 - g)):
        pl.semaphore_signal(barrier, inc=1, device_id={axis: d}, device_id_type=pl.DeviceIdType.MESH)

    mine, theirs = 512 * t, 512 * cross
    own_rows = rows(mine, 512)
    cols = own_rows
    got_x = local(0, x, XB(k))
    got_w = [local(1 + i, w, WQKV(i)) for i, w in enumerate((wq, wk, wv))]
    got_t = local(4, tab, T)
    got_gains = [local(19, gain_a_in, gain_a), local(20, gain_m_in, gain_m)]
    got_wo = local(5, wo, WO.at[own_rows])
    weights = [local(6 + i, w, to) for i, (w, to) in enumerate(((wg, WG), (wu, WU), (wd, WD)))]
    hi = remote(0, x.at[pl.ds(256, 256)], XB(k, 256, 256), sib)
    lo = remote(1, x.at[pl.ds(0, 256)], XB(k, 0, 256), sib)
    half = [256 * k + R * p for p in range(2)]
    first = [remote(2 + p, XB(0, half[p], R), XB(2, half[p], R), cross) for p in range(2)]
    direct = [remote(2 + p, x.at[pl.ds(R * p, R)], XB(2, half[p], R), cross) for p in range(2)]
    second = [remote(4 + p, XB(1, half[p], R), XB(3, half[p], R), cross) for p in range(2)]
    first_on = [remote(9 + p, XB(2, half[p], R), XB(2, half[p], R), sib) for p in range(2)]
    second_on = [remote(11 + p, XB(3, half[p], R), XB(3, half[p], R), sib) for p in range(2)]
    few = R // 2
    part = [256 * g + few * n for n in range(4)]
    wos = [remote(i, wo.at[rows(part[n], few)], WO.at[rows(mine + part[n], few)], cross) for n, i in enumerate((6, 7, 44, 45))]
    whole = remote(8, wo, WO.at[own_rows], sib)
    came = [WO.at[rows(theirs + part[n], few)] for n in range(4)]
    lent = [WO.at[rows(theirs + 256 * (1 - g) + few * n, few)] for n in range(4)]
    over = [remote(i, w, w, 1 - g, "dp") for w, i in zip(came, (13, 14, 46, 47))]
    came_on = [remote(i, w, w, sib) for w, i in zip(came, (15, 16, 48, 49))]
    lent_on = [remote(i, w, w, sib) for w, i in zip(lent, (17, 18, 50, 51))]

    def hand_on(n):
        wos[n].wait_recv()
        over[n].start()
        came_on[n].start()

    def seen(pair, p):
        i = 19 + 6 * pair + 3 * p
        to = S.at[pair, p, :, :, cols]
        return [remote(i, (TS if pair == OTH else OS).at[p], to, sib), remote(i + 1, S.at[1 - pair, p, :, :, cols], to, cross),
                remote(i + 2, (OS if pair == OTH else TS).at[p], to, diag)]

    def seen_here(pair, p):
        i = 19 + 6 * pair + 3 * p
        return [remote(i + n, OS.at[p], S.at[pair, p, :, :, cols], sib) for n in range(3)]

    def hs(pair, p):
        return remote(31 + 2 * pair + p, X.at[pair, p], HS.at[pair, p], sib)

    def away(p):
        return remote(35 + p, SA.at[p], AW.at[p], sib)

    far0 = remote(37, SF.at[0], FAR, cross)
    far_rest = [remote(n, SF.at[1, pl.ds(j * R, R)], far1.at[j], cross) for j, n in enumerate((38, 43))]

    def near(p):
        return [remote(39 + 2 * p + j, SA.at[p, pl.ds(j * R, R)], S.at[OTH, p, j], sib) for j in range(2)]

    ended = [local(9 + j, AW.at[0, pl.ds(R * j, R)], y0.at[j]) for j in range(2)]
    ended_z = [local(11 + 2 * n + j, ACC.at[n, j, pl.ds(0, R)], z1.at[j, :, pl.ds(512 * n, 512)]) for n in range(4) for j in range(2)]

    for copy in (got_x, *got_gains, *got_w, got_t, got_wo):
        copy.start()
    pl.semaphore_wait(barrier, 4)
    hi.start()
    lo.start()

    @pl.when(k == 0)
    def _():
        for copy in direct:
            copy.start()

    hi.wait_recv()

    @pl.when(k == 1)
    def _():
        for copy in first:
            copy.start()

    got_x.wait()
    lo.wait_recv()
    for copy in (*second, *wos, whole):
        copy.start()

    def qkv(block, place):
        a = _normed(XB(block)[...], gain_a[...][None])
        SA[0] = a[:M]
        SA[1] = a[M:]
        tt = T[rows(place * BLOCK, BLOCK), :]
        flip = pltpu.roll(tt, HEAD // 2, 1)
        left = lax.broadcasted_iota(jnp.int32, tt.shape, 1) < HEAD // 2
        cos, sin = jnp.where(left, tt, flip), jnp.where(left, -flip, tt)
        a = SA[...].reshape(BLOCK, 2048)
        for h in range(0, HEADS, 2):
            for i, out in enumerate((QS, KS)):
                z2 = _dot(a, WU[:, BLOCK * i + HEAD * h : BLOCK * i + HEAD * (h + 2)]).astype(BF16).astype(F32)
                for n in range(2):
                    z = z2[:, n * HEAD : (n + 1) * HEAD]
                    out(block, h + n)[...] = (z * cos + pltpu.roll(z, HEAD // 2, 1) * sin).astype(BF16)
            v = _dot(a, WU[:, 2 * BLOCK + HEAD * h : 2 * BLOCK + HEAD * (h + 2)]).astype(BF16)
            for n in range(2):
                VS(block, h + n)[...] = v[:, n * HEAD : (n + 1) * HEAD].T

    def task(n, q, kv, diagonal=False):
        return QS(q, n)[...], KS(kv, n)[...], VS(kv, n)[...], diagonal

    def either(n, j, o):
        return task(n, jnp.where(late, o, j), jnp.where(late, j, o))

    def put(pair, j, n, o):
        lo, hi = o[: BLOCK // 2], o[BLOCK // 2 :]
        e = k if j == 0 else 1 - k
        m, s = jnp.where(k == 0, lo, hi), jnp.where(k == 0, hi, lo)
        for p in range(2):
            S[pair, p, e, :, rows(mine + HEAD * n, HEAD)] = m[p * R : (p + 1) * R]
            (OS if pair == OWN else TS)[p, 1 - e, :, rows(HEAD * n, HEAD)] = s[p * R : (p + 1) * R]

    def second_phase(n, _):
        a, *b = _tasks([task(n, 0, 0, True), task(n, 1, 0), task(n, 1, 1, True)])
        for j, (acc, top) in enumerate((a, _merge(b))):
            ACC[n, j], TOP[n, j] = acc, top

    def third_phase(n, _):
        d, *f = _tasks([task(n, 2, 2, True), either(n, 0, 2), either(n, 1, 2)])
        put(OTH, 0, n, _ended(_merge([d, _if(late, f[0]), _if(late, f[1])])))
        for j in range(2):
            ACC[n, j], TOP[n, j] = _merge([(ACC[n, j], TOP[n, j]), _if(c == 1, f[j])])

    def fourth_phase(n, _):
        for piece in range(2):

            @pl.when(n == 2 * piece + 1)
            def _():
                hand_on(piece)

        d, z, *f = _tasks([task(n, 3, 3, True), task(n, 3, 2), either(n, 0, 3), either(n, 1, 3)])
        put(OTH, 1, n, _ended(_merge([d, z, _if(late, f[0]), _if(late, f[1])])))
        for j in range(2):
            put(OWN, j, n, _ended(_merge([(ACC[n, j], TOP[n, j]), _if(c == 1, f[j])])))

    def arrive(copies, on):
        for p in range(2):
            copies[p].wait_recv()
            on[p].start()
        for p in range(2):
            on[p].wait_recv()

    for copy in (*got_w, got_t, *got_gains):
        copy.wait()

    def blocks(i, _):
        @pl.when(i == 2)
        def _():
            arrive(first, first_on)

        @pl.when(i == 3)
        def _():
            arrive(second, second_on)

        own = i < 2
        block = jnp.where(own, jnp.where(i == 0, k, 1 - k), i)
        qkv(block, jnp.where(own, 2 * c + block, 2 * (1 - c) + i - 2))
        pair, e = jnp.where(own, OWN, OTH), jnp.where(own, i, jnp.where(i == 2, k, 1 - k))
        for p in range(2):
            X[pair, p, e] = XB(block, half[p], R)[...]

        for at, phase in ((1, second_phase), (2, third_phase), (3, fourth_phase)):

            @pl.when(i == at)
            def _():
                lax.fori_loop(0, HEADS, phase, None)

    lax.fori_loop(0, 4, blocks, None)
    for copy in seen(OTH, 0):
        copy.start()
    hand_on(2)
    for copy in (hi, lo, *first, *second, *first_on, *second_on):
        copy.wait_send()
    for copy in weights:
        copy.start()

    hand_on(3)
    for copy in seen(OTH, 1):
        copy.start()
    for n in range(4):
        over[n].wait_recv()
        lent_on[n].start()
    for p in range(2):
        for copy in seen(OWN, p):
            copy.start()
    got_wo.wait()
    for copy in (whole, *came_on, *lent_on):
        copy.wait_recv()
    for copy in weights:
        copy.wait()

    def h_of(pair, p):
        for copy in seen_here(pair, p):
            copy.wait_recv()
        a = S[pair, p].reshape(M, 2048)
        for n in range(0, 2048, TILE):
            at = slice(n, n + TILE)
            h = X[pair, p, :, :, at].reshape(M, TILE).astype(F32) + _dot(a, WO[:, at])
            X[pair, p, :, :, at] = h.astype(BF16).reshape(2, R, TILE)
        hs(pair, p).start()

    def down(out):
        hidden = H[...]
        for n in range(0, 2048, TILE):
            at = slice(n, n + TILE)
            out(n, at, _dot(hidden, WD[:, at]))

    def swapped(ref, p, at):
        return jnp.concatenate([ref[p, R:, at], ref[p, :R, at]], 0).astype(F32)

    def swapped_near(p, at):
        return jnp.concatenate([S[OTH, p, 1, :, at], S[OTH, p, 0, :, at]], 0).astype(F32)

    def step(i, _):
        pair, p, e = lax.div(i, 4), lax.rem(lax.div(i, 2), 2), 1 - lax.rem(i, 2)
        q = 2 * pair + 1 - e

        @pl.when(e == 1)
        def _():
            hs(pair, p).wait_recv()

        B[:R, :] = _normed(X[pair, p, e], gain_m[...][None])
        B[R:, :] = _normed(HS[pair, p, 1 - e], gain_m[...][None])
        b = B[...]
        for n in range(0, 2048, TILE):
            at = slice(n, n + TILE)
            gate, up = _dot(b, WG[:, at]), _dot(b, WU[:, at])
            H[:, at] = (gate * jax.nn.sigmoid(gate) * up).astype(BF16)

        for p_, at in ((0, 3), (1, 5)):

            @pl.when(i == at)
            def _():
                for copy in (*seen(OTH, p_), *seen(OWN, p_)):
                    copy.wait_send()

        @pl.when((i == 1) | (i == 3) | (i == 5))
        def _():
            h_of(jnp.where(i == 1, OTH, OWN), jnp.where(i == 3, 0, 1))

        @pl.when(e == 1)
        def _():
            @pl.when(q == 2)
            def _():
                away(p).wait_send()

            def out(n, at, term):
                SA[p, :, at] = term.astype(BF16)

            down(out)

            @pl.when(q == 0)
            def _():
                away(p).start()

            @pl.when(q == 2)
            def _():
                for copy in near(p):
                    copy.start()

        @pl.when(q == 1)
        def _():
            away(p).wait_recv()

            def out(n, at, term):
                SF[p, :, at] = (term + swapped(AW, p, at)).astype(BF16)

            down(out)

            @pl.when(p == 0)
            def _():
                far0.start()

            @pl.when(p == 1)
            def _():
                for copy in far_rest:
                    copy.start()

        @pl.when(q == 3)
        def _():
            for copy in near(p):
                copy.wait_recv()

            def out(n, at, term):
                h = jnp.concatenate([X[OWN, p, 0, :, at], HS[OWN, p, 1, :, at]], 0).astype(F32)
                z = h + term + swapped_near(p, at)
                for j in range(2):
                    ACC[n // 512, j, :HEAD, n % 512 : n % 512 + TILE] = z[j * R : (j + 1) * R]

            down(out)

            @pl.when(p == 0)
            def _():
                far0.wait_recv()
                for n in range(0, 2048, 512):
                    for j in range(2):
                        r, at = slice(j * R, (j + 1) * R), slice(n, n + 512)
                        AW[0, r, at] = (ACC[n // 512, j, :HEAD, :] + FAR[r, at].astype(F32)).astype(BF16)
                for copy in ended:
                    copy.start()
                for copy in ended:
                    copy.wait()

            @pl.when(p == 1)
            def _():
                for copy in ended_z:
                    copy.start()

    h_of(OTH, 0)
    lax.fori_loop(0, 8, step, None)
    for copy in (*wos, whole, *over, *came_on, *lent_on):
        copy.wait_send()
    for pair in (OTH, OWN):
        for p in range(2):
            hs(pair, p).wait_send()
    far0.wait_send()
    for copy in far_rest:
        copy.wait()
    for p in range(2):
        for copy in near(p):
            copy.wait_send()
    for copy in ended_z:
        copy.wait()


def _layer(*ins):
    hbm = pl.BlockSpec(memory_space=pl.ANY)
    weight = pltpu.VMEM((2048, 2048), BF16)
    pairs = pltpu.VMEM((2, 2, 2, R, 2048), BF16)
    block = pltpu.VMEM((M, 2048), BF16)
    blocks = pltpu.VMEM((2, M, 2048), BF16)
    piece = pltpu.VMEM((2, 2, R, HEADS * HEAD), BF16)
    return pl.pallas_call(
        _body,
        in_specs=[hbm] * len(ins),
        out_specs=[hbm] * 3,
        out_shape=[jax.ShapeDtypeStruct((2, R, 2048), d) for d in (BF16, F32, BF16)],
        scratch_shapes=[*[weight] * 4, *[pairs] * 3, block, block, *[blocks] * 3, block, piece, piece, pltpu.VMEM((2048, HEAD), F32),
                        pltpu.VMEM((HEADS, 2, HEAD + 8, BLOCK), F32), pltpu.VMEM((HEADS, 2, 1, BLOCK), F32), *[pltpu.VMEM((2048,), BF16)] * 2,
                        pltpu.SemaphoreType.DMA((21,)), pltpu.SemaphoreType.DMA((52,)), pltpu.SemaphoreType.DMA((52,))],
        compiler_params=pltpu.CompilerParams(collective_id=1, has_side_effects=True, vmem_limit_bytes=67_043_328),
        cost_estimate=pl.CostEstimate(flops=2 * 2048**3 * 4, transcendentals=2**23, bytes_accessed=2**26),
        name="layer",
    )(*ins)


def _end_body(y0, z1, far1, y, A, Z, F, rsem, wsem):
    k = lax.rem(lax.axis_index("tp"), 2)
    loads = [pltpu.make_async_copy(a, b, rsem.at[3 * j + i])
             for j in range(2) for i, (a, b) in enumerate(((z1.at[j], Z.at[j]), (far1.at[j], F.at[j]), (y0.at[j], A.at[0, j])))]
    stores = [pltpu.make_async_copy(A.at[p, j], y.at[pl.ds(pl.multiple_of(256 * (k if j == 0 else 1 - k) + R * p, R), R)], wsem.at[2 * p + j])
              for p in range(2) for j in range(2)]
    for copy in loads:
        copy.start()
    for j in range(2):
        loads[3 * j].wait()
        loads[3 * j + 1].wait()
        A[1, j] = (Z[j] + F[j].astype(F32)).astype(BF16)
        stores[2 + j].start()
        loads[3 * j + 2].wait()
        stores[j].start()
    for copy in stores:
        copy.wait()


def _end(*ins):
    hbm = pl.BlockSpec(memory_space=pl.ANY)
    return pl.pallas_call(
        _end_body,
        in_specs=[hbm] * 3,
        out_specs=hbm,
        out_shape=jax.ShapeDtypeStruct((512, 2048), BF16),
        scratch_shapes=[pltpu.VMEM((2, 2, R, 2048), BF16), pltpu.VMEM((2, R, 2048), F32), pltpu.VMEM((2, R, 2048), BF16),
                        pltpu.SemaphoreType.DMA((6,)), pltpu.SemaphoreType.DMA((4,))],
        compiler_params=pltpu.CompilerParams(vmem_limit_bytes=67_043_328),
        cost_estimate=pl.CostEstimate(flops=2**20, transcendentals=0, bytes_accessed=6 * 2**20),
        name="end",
    )(*ins)


def solution(mesh):
    def step(x, gain_a, wq, wk, wv, wo, gain_m, w_gate, w_up, w_down):
        return _end(*_layer(gain_a, gain_m, x, wq, wk, wv, wo, jnp.asarray(_table()), w_gate, w_up, w_down))

    tokens, columns, rows_of = P(("dp", "tp"), None), P(None, "tp"), P("tp", None)
    return jax.shard_map(
        step,
        mesh=mesh,
        in_specs=(tokens, P(None), columns, columns, columns, rows_of, P(None), columns, columns, rows_of),
        out_specs=tokens,
        check_vma=False,
    )
```

```python
import functools

import jax
import jax.numpy as jnp
import numpy as np
from jax import lax
from jax.experimental import pallas as pl
from jax.experimental.pallas import tpu as pltpu
from jax.sharding import PartitionSpec as P

HEAD = 128
HEADS = 4
BLOCK = 512
THETA = 10000
NEG = -1e30
HIDDEN = 2 * NEG
LOG2E = 1.4426950408889634
F32, BF16 = jnp.float32, jnp.bfloat16


def _dot(a, b, ca=1, cb=0):
    return lax.dot_general(a, b, (((ca,), (cb,)), ((), ())), preferred_element_type=F32)


def _normed(x, gain):
    wide = x.astype(F32)
    scale = lax.rsqrt(jnp.mean(wide * wide, -1, keepdims=True) + 1e-6)
    return (wide * scale * gain.astype(F32)).astype(BF16)


def _table():
    half = HEAD // 2
    rate = np.float32(THETA) ** (-np.arange(half, dtype=np.float32) / np.float32(half))
    angle = np.arange(2048, dtype=np.float32)[:, None] * rate.astype(np.float32)
    return np.concatenate([np.cos(angle), np.sin(angle)], 1).astype(np.float32)


E = HEAD**-0.5 * LOG2E


def _scores(q, k, diagonal):
    s = _dot(k, q, 1, 1)
    if diagonal:
        s = jnp.where(lax.broadcasted_iota(jnp.int32, s.shape, 1) >= lax.broadcasted_iota(jnp.int32, s.shape, 0), s, HIDDEN)
    return s


def _tasks(tasks):
    scores = [_scores(q, k, d) for q, k, _, d in tasks]
    out = []
    for (_, _, v, _), s in zip(tasks, scores):
        top = s.max(axis=0, keepdims=True)
        p = jnp.exp2((s - top) * E).astype(BF16)
        out.append((p, top))
    ones = jnp.ones((8, BLOCK), BF16)
    return [(_dot(jnp.concatenate([v, ones], 0), p), top) for (_, _, v, _), (p, top) in zip(tasks, out)]


def _merge(parts):
    top = functools.reduce(jnp.maximum, [t for _, t in parts])
    return sum(a * jnp.exp2((t - top) * E) for a, t in parts), top


def _if(ok, part):
    return part[0], jnp.where(ok, part[1], NEG)


def _ended(part):
    acc = part[0]
    return (acc[:HEAD] * (1 / acc[HEAD : HEAD + 1])).T.astype(BF16)


HB = 1
R = 128
M = 2 * R
TILE = 256
OTH, OWN = 0, 1


def _body(gain_a_in, gain_m_in, x, wq, wk, wv, wo, tab, wg, wu, wd, y0, z1, far1, WO, WG, WU, WD, S, X, HS, B, H, SA, SF, AW, FAR, OS, TS, T, ACC, TOP,
          gain_a, gain_m, lsem, ssem, rsem):
    t, g = lax.axis_index("tp"), lax.axis_index("dp")
    c, k = lax.div(t, 2), lax.rem(t, 2)
    sib, cross, diag = t + 1 - 2 * k, lax.rem(t + 2, 4), 3 - t
    late = c == 0

    def rows(at, n):
        return pl.ds(pl.multiple_of(at, min(n, R)), n)

    XB = lambda b, at=0, n=BLOCK: WD.at[rows(BLOCK * b + at, n)]
    WQKV = lambda i: WU.at[:, pl.ds(BLOCK * i, BLOCK)]
    KS = lambda b, n: WG.at[rows(BLOCK * b, BLOCK), rows(HEAD * n, HEAD)]
    QS = lambda b, n: WG.at[rows(BLOCK * b, BLOCK), rows(2 * BLOCK + HEAD * n, HEAD)]
    VS = lambda b, n: WG.at[rows(BLOCK * b + HEAD * n, HEAD), pl.ds(BLOCK, BLOCK)]

    def local(i, src, dst):
        return pltpu.make_async_copy(src, dst, lsem.at[i])

    def remote(i, src, dst, to, axis="tp"):
        return pltpu.make_async_remote_copy(
            src, dst, ssem.at[i], rsem.at[i], device_id={axis: to}, device_id_type=pl.DeviceIdType.MESH)

    barrier = pltpu.get_barrier_semaphore()
    for axis, d in (("tp", sib), ("tp", cross), ("tp", diag), ("dp", 1 - g)):
        pl.semaphore_signal(barrier, inc=1, device_id={axis: d}, device_id_type=pl.DeviceIdType.MESH)

    mine, theirs = 512 * t, 512 * cross
    own_rows = rows(mine, 512)
    cols = own_rows
    got_x = local(0, x, XB(k))
    got_w = [local(1 + i, w, WQKV(i)) for i, w in enumerate((wq, wk, wv))]
    got_t = local(4, tab, T)
    got_gains = [local(19, gain_a_in, gain_a), local(20, gain_m_in, gain_m)]
    got_wo = local(5, wo, WO.at[own_rows])
    weights = [local(6 + i, w, to) for i, (w, to) in enumerate(((wg, WG), (wu, WU), (wd, WD)))]
    hi = remote(0, XB(k, 256, 256), XB(k, 256, 256), sib)
    lo = remote(1, XB(k, 0, 256), XB(k, 0, 256), sib)
    half = [256 * k + R * p for p in range(2)]
    first = [remote(2 + p, XB(0, half[p], R), XB(2, half[p], R), cross) for p in range(2)]
    second = [remote(4 + p, XB(1, half[p], R), XB(3, half[p], R), cross) for p in range(2)]
    first_on = [remote(9 + p, XB(2, half[p], R), XB(2, half[p], R), sib) for p in range(2)]
    second_on = [remote(11 + p, XB(3, half[p], R), XB(3, half[p], R), sib) for p in range(2)]
    few = R // 2
    part = [256 * g + few * n for n in range(4)]
    wos = [remote(i, wo.at[rows(part[n], few)], WO.at[rows(mine + part[n], few)], cross) for n, i in enumerate((6, 7, 44, 45))]
    whole = remote(8, wo, WO.at[own_rows], sib)
    came = [WO.at[rows(theirs + part[n], few)] for n in range(4)]
    lent = [WO.at[rows(theirs + 256 * (1 - g) + few * n, few)] for n in range(4)]
    over = [remote(i, w, w, 1 - g, "dp") for w, i in zip(came, (13, 14, 46, 47))]
    came_on = [remote(i, w, w, sib) for w, i in zip(came, (15, 16, 48, 49))]
    lent_on = [remote(i, w, w, sib) for w, i in zip(lent, (17, 18, 50, 51))]

    def hand_on(n):
        wos[n].wait_recv()
        over[n].start()
        came_on[n].start()

    def seen(pair, p):
        i = 19 + 6 * pair + 3 * p
        to = S.at[pair, p, :, :, cols]
        return [remote(i, (TS if pair == OTH else OS).at[p], to, sib), remote(i + 1, S.at[1 - pair, p, :, :, cols], to, cross),
                remote(i + 2, (OS if pair == OTH else TS).at[p], to, diag)]

    def seen_here(pair, p):
        i = 19 + 6 * pair + 3 * p
        return [remote(i + n, OS.at[p], S.at[pair, p, :, :, cols], sib) for n in range(3)]

    def hs(pair, p):
        return remote(31 + 2 * pair + p, X.at[pair, p], HS.at[pair, p], sib)

    def away(p):
        return remote(35 + p, SA.at[p], AW.at[p], sib)

    far0 = remote(37, SF.at[0], FAR, cross)
    far_rest = [remote(n, SF.at[1, pl.ds(j * R, R)], far1.at[j], cross) for j, n in enumerate((38, 43))]

    def near(p):
        return [remote(39 + 2 * p + j, SA.at[p, pl.ds(j * R, R)], S.at[OTH, p, j], sib) for j in range(2)]

    ended = [local(9 + j, AW.at[0, pl.ds(R * j, R)], y0.at[j]) for j in range(2)]
    ended_z = [local(11 + 2 * n + j, ACC.at[n, j, pl.ds(0, R)], z1.at[j, :, pl.ds(512 * n, 512)]) for n in range(4) for j in range(2)]

    for copy in (got_x, *got_gains, *got_w, got_t, got_wo):
        copy.start()
    got_x.wait()
    pl.semaphore_wait(barrier, 4)

    @pl.when(k == 0)
    def _():
        for copy in first:
            copy.start()

    hi.start()
    lo.start()
    hi.wait_recv()

    @pl.when(k == 1)
    def _():
        for copy in first:
            copy.start()

    lo.wait_recv()
    for copy in (*second, *wos, whole):
        copy.start()

    def qkv(block, place):
        a = _normed(XB(block)[...], gain_a[...][None])
        SA[0] = a[:M]
        SA[1] = a[M:]
        tt = T[rows(place * BLOCK, BLOCK), :]
        flip = pltpu.roll(tt, HEAD // 2, 1)
        left = lax.broadcasted_iota(jnp.int32, tt.shape, 1) < HEAD // 2
        cos, sin = jnp.where(left, tt, flip), jnp.where(left, -flip, tt)
        a = SA[...].reshape(BLOCK, 2048)
        for h in range(0, HEADS, 2):
            for i, out in enumerate((QS, KS)):
                z2 = _dot(a, WU[:, BLOCK * i + HEAD * h : BLOCK * i + HEAD * (h + 2)]).astype(BF16).astype(F32)
                for n in range(2):
                    z = z2[:, n * HEAD : (n + 1) * HEAD]
                    out(block, h + n)[...] = (z * cos + pltpu.roll(z, HEAD // 2, 1) * sin).astype(BF16)
            v = _dot(a, WU[:, 2 * BLOCK + HEAD * h : 2 * BLOCK + HEAD * (h + 2)]).astype(BF16)
            for n in range(2):
                VS(block, h + n)[...] = v[:, n * HEAD : (n + 1) * HEAD].T

    def task(n, q, kv, diagonal=False):
        return QS(q, n)[...], KS(kv, n)[...], VS(kv, n)[...], diagonal

    def either(n, j, o):
        return task(n, jnp.where(late, o, j), jnp.where(late, j, o))

    def put(pair, j, n, o):
        lo, hi = o[: BLOCK // 2], o[BLOCK // 2 :]
        e = k if j == 0 else 1 - k
        m, s = jnp.where(k == 0, lo, hi), jnp.where(k == 0, hi, lo)
        for p in range(2):
            S[pair, p, e, :, rows(mine + HEAD * n, HEAD)] = m[p * R : (p + 1) * R]
            (OS if pair == OWN else TS)[p, 1 - e, :, rows(HEAD * n, HEAD)] = s[p * R : (p + 1) * R]

    def second_phase(n, _):
        a, *b = _tasks([task(n, 0, 0, True), task(n, 1, 0), task(n, 1, 1, True)])
        for j, (acc, top) in enumerate((a, _merge(b))):
            ACC[n, j], TOP[n, j] = acc, top

    def third_phase(n, _):
        d, *f = _tasks([task(n, 2, 2, True), either(n, 0, 2), either(n, 1, 2)])
        put(OTH, 0, n, _ended(_merge([d, _if(late, f[0]), _if(late, f[1])])))
        for j in range(2):
            ACC[n, j], TOP[n, j] = _merge([(ACC[n, j], TOP[n, j]), _if(c == 1, f[j])])

    def fourth_phase(n, _):
        for piece in range(2):

            @pl.when(n == 2 * piece + 1)
            def _():
                hand_on(piece)

        d, z, *f = _tasks([task(n, 3, 3, True), task(n, 3, 2), either(n, 0, 3), either(n, 1, 3)])
        put(OTH, 1, n, _ended(_merge([d, z, _if(late, f[0]), _if(late, f[1])])))
        for j in range(2):
            put(OWN, j, n, _ended(_merge([(ACC[n, j], TOP[n, j]), _if(c == 1, f[j])])))

    def arrive(copies, on):
        for p in range(2):
            copies[p].wait_recv()
            on[p].start()
        for p in range(2):
            on[p].wait_recv()

    for copy in (*got_w, got_t, *got_gains):
        copy.wait()

    def blocks(i, _):
        @pl.when(i == 2)
        def _():
            arrive(first, first_on)

        @pl.when(i == 3)
        def _():
            arrive(second, second_on)

        own = i < 2
        block = jnp.where(own, jnp.where(i == 0, k, 1 - k), i)
        qkv(block, jnp.where(own, 2 * c + block, 2 * (1 - c) + i - 2))
        pair, e = jnp.where(own, OWN, OTH), jnp.where(own, i, jnp.where(i == 2, k, 1 - k))
        for p in range(2):
            X[pair, p, e] = XB(block, half[p], R)[...]

        for at, phase in ((1, second_phase), (2, third_phase), (3, fourth_phase)):

            @pl.when(i == at)
            def _():
                lax.fori_loop(0, HEADS, phase, None)

    lax.fori_loop(0, 4, blocks, None)
    for copy in seen(OTH, 0):
        copy.start()
    hand_on(2)
    for copy in (hi, lo, *first, *second, *first_on, *second_on):
        copy.wait_send()
    for copy in weights:
        copy.start()

    hand_on(3)
    for copy in seen(OTH, 1):
        copy.start()
    for n in range(4):
        over[n].wait_recv()
        lent_on[n].start()
    for p in range(2):
        for copy in seen(OWN, p):
            copy.start()
    got_wo.wait()
    for copy in (whole, *came_on, *lent_on):
        copy.wait_recv()
    for copy in weights:
        copy.wait()

    def h_of(pair, p):
        for copy in seen_here(pair, p):
            copy.wait_recv()
        a = S[pair, p].reshape(M, 2048)
        for n in range(0, 2048, TILE):
            at = slice(n, n + TILE)
            h = X[pair, p, :, :, at].reshape(M, TILE).astype(F32) + _dot(a, WO[:, at])
            X[pair, p, :, :, at] = h.astype(BF16).reshape(2, R, TILE)
        hs(pair, p).start()

    def down(out):
        hidden = H[...]
        for n in range(0, 2048, TILE):
            at = slice(n, n + TILE)
            out(n, at, _dot(hidden, WD[:, at]))

    def swapped(ref, p, at):
        return jnp.concatenate([ref[p, R:, at], ref[p, :R, at]], 0).astype(F32)

    def swapped_near(p, at):
        return jnp.concatenate([S[OTH, p, 1, :, at], S[OTH, p, 0, :, at]], 0).astype(F32)

    def step(i, _):
        pair, p, e = lax.div(i, 4), lax.rem(lax.div(i, 2), 2), 1 - lax.rem(i, 2)
        q = 2 * pair + 1 - e

        @pl.when(e == 1)
        def _():
            hs(pair, p).wait_recv()

        B[:R, :] = _normed(X[pair, p, e], gain_m[...][None])
        B[R:, :] = _normed(HS[pair, p, 1 - e], gain_m[...][None])
        b = B[...]
        for n in range(0, 2048, TILE):
            at = slice(n, n + TILE)
            gate, up = _dot(b, WG[:, at]), _dot(b, WU[:, at])
            H[:, at] = (gate * jax.nn.sigmoid(gate) * up).astype(BF16)

        for p_, at in ((0, 3), (1, 5)):

            @pl.when(i == at)
            def _():
                for copy in (*seen(OTH, p_), *seen(OWN, p_)):
                    copy.wait_send()

        @pl.when((i == 1) | (i == 3) | (i == 5))
        def _():
            h_of(jnp.where(i == 1, OTH, OWN), jnp.where(i == 3, 0, 1))

        @pl.when(e == 1)
        def _():
            @pl.when(q == 2)
            def _():
                away(p).wait_send()

            def out(n, at, term):
                SA[p, :, at] = term.astype(BF16)

            down(out)

            @pl.when(q == 0)
            def _():
                away(p).start()

            @pl.when(q == 2)
            def _():
                for copy in near(p):
                    copy.start()

        @pl.when(q == 1)
        def _():
            away(p).wait_recv()

            def out(n, at, term):
                SF[p, :, at] = (term + swapped(AW, p, at)).astype(BF16)

            down(out)

            @pl.when(p == 0)
            def _():
                far0.start()

            @pl.when(p == 1)
            def _():
                for copy in far_rest:
                    copy.start()

        @pl.when(q == 3)
        def _():
            for copy in near(p):
                copy.wait_recv()

            def out(n, at, term):
                h = jnp.concatenate([X[OWN, p, 0, :, at], HS[OWN, p, 1, :, at]], 0).astype(F32)
                z = h + term + swapped_near(p, at)
                for j in range(2):
                    ACC[n // 512, j, :HEAD, n % 512 : n % 512 + TILE] = z[j * R : (j + 1) * R]

            down(out)

            @pl.when(p == 0)
            def _():
                far0.wait_recv()
                for n in range(0, 2048, 512):
                    for j in range(2):
                        r, at = slice(j * R, (j + 1) * R), slice(n, n + 512)
                        AW[0, r, at] = (ACC[n // 512, j, :HEAD, :] + FAR[r, at].astype(F32)).astype(BF16)
                for copy in ended:
                    copy.start()
                for copy in ended:
                    copy.wait()

            @pl.when(p == 1)
            def _():
                for copy in ended_z:
                    copy.start()

    h_of(OTH, 0)
    lax.fori_loop(0, 8, step, None)
    for copy in (*wos, whole, *over, *came_on, *lent_on):
        copy.wait_send()
    for pair in (OTH, OWN):
        for p in range(2):
            hs(pair, p).wait_send()
    far0.wait_send()
    for copy in far_rest:
        copy.wait()
    for p in range(2):
        for copy in near(p):
            copy.wait_send()
    for copy in ended_z:
        copy.wait()


def _layer(*ins):
    hbm = pl.BlockSpec(memory_space=pl.ANY)
    weight = pltpu.VMEM((2048, 2048), BF16)
    pairs = pltpu.VMEM((2, 2, 2, R, 2048), BF16)
    block = pltpu.VMEM((M, 2048), BF16)
    blocks = pltpu.VMEM((2, M, 2048), BF16)
    piece = pltpu.VMEM((2, 2, R, HEADS * HEAD), BF16)
    return pl.pallas_call(
        _body,
        in_specs=[hbm] * len(ins),
        out_specs=[hbm] * 3,
        out_shape=[jax.ShapeDtypeStruct((2, R, 2048), d) for d in (BF16, F32, BF16)],
        scratch_shapes=[*[weight] * 4, *[pairs] * 3, block, block, *[blocks] * 3, block, piece, piece, pltpu.VMEM((2048, HEAD), F32),
                        pltpu.VMEM((HEADS, 2, HEAD + 8, BLOCK), F32), pltpu.VMEM((HEADS, 2, 1, BLOCK), F32), *[pltpu.VMEM((2048,), BF16)] * 2,
                        pltpu.SemaphoreType.DMA((21,)), pltpu.SemaphoreType.DMA((52,)), pltpu.SemaphoreType.DMA((52,))],
        compiler_params=pltpu.CompilerParams(collective_id=1, has_side_effects=True, vmem_limit_bytes=67_043_328),
        cost_estimate=pl.CostEstimate(flops=2 * 2048**3 * 4, transcendentals=2**23, bytes_accessed=2**26),
        name="layer",
    )(*ins)


def _end_body(y0, z1, far1, y, A, Z, F, rsem, wsem):
    k = lax.rem(lax.axis_index("tp"), 2)
    loads = [pltpu.make_async_copy(a, b, rsem.at[3 * j + i])
             for j in range(2) for i, (a, b) in enumerate(((z1.at[j], Z.at[j]), (far1.at[j], F.at[j]), (y0.at[j], A.at[0, j])))]
    stores = [pltpu.make_async_copy(A.at[p, j], y.at[pl.ds(pl.multiple_of(256 * (k if j == 0 else 1 - k) + R * p, R), R)], wsem.at[2 * p + j])
              for p in range(2) for j in range(2)]
    for copy in loads:
        copy.start()
    for j in range(2):
        loads[3 * j].wait()
        loads[3 * j + 1].wait()
        A[1, j] = (Z[j] + F[j].astype(F32)).astype(BF16)
        stores[2 + j].start()
        loads[3 * j + 2].wait()
        stores[j].start()
    for copy in stores:
        copy.wait()


def _end(*ins):
    hbm = pl.BlockSpec(memory_space=pl.ANY)
    return pl.pallas_call(
        _end_body,
        in_specs=[hbm] * 3,
        out_specs=hbm,
        out_shape=jax.ShapeDtypeStruct((512, 2048), BF16),
        scratch_shapes=[pltpu.VMEM((2, 2, R, 2048), BF16), pltpu.VMEM((2, R, 2048), F32), pltpu.VMEM((2, R, 2048), BF16),
                        pltpu.SemaphoreType.DMA((6,)), pltpu.SemaphoreType.DMA((4,))],
        compiler_params=pltpu.CompilerParams(vmem_limit_bytes=67_043_328),
        cost_estimate=pl.CostEstimate(flops=2**20, transcendentals=0, bytes_accessed=6 * 2**20),
        name="end",
    )(*ins)


def solution(mesh):
    def step(x, gain_a, wq, wk, wv, wo, gain_m, w_gate, w_up, w_down):
        return _end(*_layer(gain_a, gain_m, x, wq, wk, wv, wo, jnp.asarray(_table()), w_gate, w_up, w_down))

    tokens, columns, rows_of = P(("dp", "tp"), None), P(None, "tp"), P("tp", None)
    return jax.shard_map(
        step,
        mesh=mesh,
        in_specs=(tokens, P(None), columns, columns, columns, rows_of, P(None), columns, columns, rows_of),
        out_specs=tokens,
        check_vma=False,
    )
```
